32 devices in a mesh: row: 4 (over y, core), col: 8 (over z, x).
Axes of the slice: x: 2, y: 2, z: 4, core: 2. Of those that a mesh axis runs over, the one named last changes fastest.
Arguments:
- values: bfloat16 [8192, 128], P('row'), may hold values from -30 to 30
- points0: bfloat16 [2, 8192], P(None, 'row'), may hold values from 0 to 1
- points1: bfloat16 [2, 2048], P(None, 'row'), may hold values from 0 to 1
- points2: bfloat16 [2, 256], P(None, 'row'), may hold values from 0 to 1
- tiles_a0: int32 [4, 8, 2, 48], P('row', 'col'), may hold values from 0 to 15, as said below
- tiles_e1: int32 [4, 8, 2, 20], P('row', 'col'), may hold values from 0 to 15, as said below
- tiles_a1: int32 [4, 8, 2, 4], P('row', 'col'), may hold values from 0 to 3, as said below
- factor: bfloat16 [256, 256], P('row', 'col'), as said below
Outputs:
- fine_coef: float32 [8192, 128], P(('row', 'col'))
- mid_coef: float32 [2048, 128], P('col')
- coarse_coef: float32 [256, 128], P('row')
- norms: float32 [1], replicated
The draws below stay inside these ranges and needn't reach their ends.
Inputs may be any that keep to these rules, and one draw needn't show every extreme that they name: `tiles_a0`: within each block the 48 listed tile pairs are distinct; tile rows are below 16 and tile columns below 8. `tiles_e1`: within each block the 20 listed tile pairs are distinct; tile rows are below 16 and tile columns below 2. `tiles_a1`: within each block the 4 listed tile pairs are distinct; tile rows are below 4 and tile columns below 2. `factor`: upper triangular; diagonal entries from 1 to 2.
All inputs are finite; a program needn't handle non-finite values.
Results may differ from the reference program's by a relative error of at most 0.0042.
Values may be sent and summed in bfloat16 or wider, within the bound.
A program may use at most 64 MiB of HBM per device.

```python
import jax
import jax.numpy as jnp
from jax import lax

TILE = 128
FIELDS = 128
N0 = 8192
N1 = 2048
N2 = 256
ROWS0 = 2048
COLS0 = 1024
ROWS1 = 512
COLS1 = 256
ROWS2 = 64
MAXT_A0 = 48
MAXT_E1 = 20
MAXT_A1 = 4
N_ROW = 4
N_COL = 8


def pick_tiles(key, stream, row_range, col_range, listed):
    subkeys = jax.random.split(jax.random.fold_in(key, stream), N_ROW * N_COL)

    def choose_one(subkey):
        return jax.random.permutation(subkey, row_range * col_range)[:listed]
    chosen = jax.vmap(choose_one)(subkeys).astype(jnp.int32)
    chosen = chosen.reshape(N_ROW, N_COL, 1, listed)
    return jnp.concatenate([chosen // col_range, chosen % col_range], axis=2)


def draw_values(key, part):
    base = jax.random.fold_in(key, 505)
    entry_key, row_key = jax.random.split(base)
    position = jnp.arange(N0, dtype=jnp.float32) / N0
    jitter = jnp.exp(jax.random.uniform(row_key, (N0,), jnp.float32, -0.22, 0.22))
    entries = jnp.clip(jax.random.normal(entry_key, (N0, FIELDS), jnp.float32), -6.0, 6.0)
    scale = jnp.exp(position * jnp.log(3.5)) * jitter
    return (entries * scale[:, None]).astype(jnp.bfloat16)


def draw_tiles_a0(key, part):
    return pick_tiles(key, 101, ROWS0 // TILE, COLS0 // TILE, MAXT_A0)


def draw_tiles_e1(key, part):
    return pick_tiles(key, 202, ROWS0 // TILE, COLS1 // TILE, MAXT_E1)


def draw_tiles_a1(key, part):
    return pick_tiles(key, 303, ROWS1 // TILE, COLS1 // TILE, MAXT_A1)


def draw_factor(key, part):
    base = jax.random.fold_in(key, 404)
    diag_key, upper_key = jax.random.split(base)
    index = jnp.arange(N2)
    upper = index[None, :] > index[:, None]
    spread = jax.random.normal(upper_key, (N2, N2), jnp.float32)
    diagonal = jax.random.uniform(diag_key, (N2,), jnp.float32, 1.0, 2.0)
    matrix = jnp.where(upper, spread * (0.6 / N2 ** 0.5), 0.0) + jnp.diag(diagonal)
    return matrix.astype(jnp.bfloat16)


def shard_levels(stream_key, extent, pieces, smallest, top_value):
    factor_of, own = 1.0, jax.random.fold_in(stream_key, 6)
    for dim, shards_of in pieces:
        steps = jnp.exp(jax.random.uniform(jax.random.fold_in(own, dim), (shards_of,), jnp.float32, smallest / len(pieces), top_value / len(pieces)))
        factor_of = factor_of * jnp.repeat(steps, extent[dim] // shards_of).reshape([-1 if axis == dim else 1 for axis in range(len(extent))])
    return factor_of


def setup_inputs(seed: int = 0) -> dict:
    key_of = jax.random.split(jax.random.key(seed), 9)
    return {
        "values": draw_values(jax.random.fold_in(key_of[8], 71), 0),
        "points0": jnp.clip(1.0 * jax.random.uniform(key_of[1], (2, N0), jnp.float32) ** shard_levels(key_of[1], (2, N0), ((1, 4),), -0.2, 0.2), 0.0, 1.0).astype(jnp.bfloat16),
        "points1": jnp.clip(1.0 * jax.random.uniform(key_of[2], (2, N1), jnp.float32) ** shard_levels(key_of[2], (2, N1), ((1, 4),), -0.2, 0.2), 0.0, 1.0).astype(jnp.bfloat16),
        "points2": jnp.clip(1.0 * jax.random.uniform(key_of[3], (2, N2), jnp.float32) ** shard_levels(key_of[3], (2, N2), ((1, 4),), -0.2, 0.2), 0.0, 1.0).astype(jnp.bfloat16),
        "tiles_a0": draw_tiles_a0(jax.random.fold_in(key_of[8], 71), 0),
        "tiles_e1": draw_tiles_e1(jax.random.fold_in(key_of[8], 71), 0),
        "tiles_a1": draw_tiles_a1(jax.random.fold_in(key_of[8], 71), 0),
        "factor": draw_factor(jax.random.fold_in(key_of[8], 71), 0),
    }


support_fine = 0.35
support_mid = 0.55
support_coarse = 0.8

def wendland(left_pts, right_pts, support):
    left = left_pts.astype(jnp.float32)
    right = right_pts.astype(jnp.float32)
    across = left[0][..., :, None] - right[0][..., None, :]
    upward = left[1][..., :, None] - right[1][..., None, :]
    ratio_t = jnp.sqrt(across * across + upward * upward) / support
    margin = jnp.maximum(1.0 - ratio_t, 0.0)
    squared = margin * margin
    return (squared * squared * (4.0 * ratio_t + 1.0)).astype(jnp.bfloat16)

def listed_all(row_pts, col_pts, listing, vector, support, flipped):
    row_tiles = row_pts.reshape(2, -1, TILE)
    col_tiles = col_pts.reshape(2, -1, TILE)
    rows_block = row_tiles.shape[1] // N_ROW
    cols_block = col_tiles.shape[1] // N_COL
    row_start = (jnp.arange(N_ROW, dtype=jnp.int32) * rows_block)[:, None, None]
    col_start = (jnp.arange(N_COL, dtype=jnp.int32) * cols_block)[None, :, None]
    global_rows = (listing[:, :, 0, :].astype(jnp.int32) + row_start).reshape(N_ROW * N_COL, -1)
    global_cols = (listing[:, :, 1, :].astype(jnp.int32) + col_start).reshape(N_ROW * N_COL, -1)
    fields = vector.shape[-1]
    inputs = vector.astype(jnp.float32).reshape(-1, TILE, fields)
    target = col_tiles.shape[1] if flipped else row_tiles.shape[1]
    total = jnp.zeros((target, TILE, fields), jnp.float32)

    def add_block(total, pair):
        tile_rows, tile_cols = pair
        kernel = wendland(row_tiles[:, tile_rows], col_tiles[:, tile_cols], support).astype(jnp.float32)
        if flipped:
            contrib = jnp.einsum('gij,gir->gjr', kernel, inputs[tile_rows])
            return (total.at[tile_cols].add(contrib), None)
        contrib = jnp.einsum('gij,gjr->gir', kernel, inputs[tile_cols])
        return (total.at[tile_rows].add(contrib), None)
    total, unused = lax.scan(add_block, total, (global_rows, global_cols))
    return total.reshape(-1, fields)

def reference(values, points0, points1, points2, tiles_a0, tiles_e1, tiles_a1, factor):
    scale_a0 = (ROWS0 / (N_COL * MAXT_A0 * TILE * TILE)) ** 0.5
    scale_e1 = (ROWS0 / (N_COL * MAXT_E1 * TILE * TILE)) ** 0.5
    scale_a1 = (ROWS1 / (N_COL * MAXT_A1 * TILE * TILE)) ** 0.5
    scale_e2 = (1.0 / N1) ** 0.5
    fine_data = values.astype(jnp.float32)
    fine_res = fine_data - 0.5 * (scale_a0 * listed_all(points0, points0, tiles_a0, values, support_fine, False))
    mid_data = scale_e1 * listed_all(points0, points1, tiles_e1, fine_res.astype(jnp.bfloat16), support_mid, True)
    mid_prod = (scale_a1 * listed_all(points1, points1, tiles_a1, mid_data.astype(jnp.bfloat16), support_mid, False)).astype(jnp.bfloat16)
    mid_res = mid_data - 0.5 * mid_prod.astype(jnp.float32)
    mid_low = mid_res.astype(jnp.bfloat16)
    coarse_blocks = points2.reshape(2, N_ROW, ROWS2).transpose(1, 0, 2)

    def restrict_block(block_pts):
        kernel = wendland(block_pts, points1, support_coarse)
        return jnp.dot(kernel, mid_low, preferred_element_type=jnp.float32)
    coarse_raw = lax.map(restrict_block, coarse_blocks).reshape(N2, -1)
    coarse_data = (scale_e2 * coarse_raw).astype(jnp.bfloat16)
    halfway = jnp.dot(factor.T, coarse_data, preferred_element_type=jnp.float32).astype(jnp.bfloat16)
    coarse_coef = jnp.dot(factor, halfway, preferred_element_type=jnp.float32)
    coarse_low = coarse_coef.astype(jnp.bfloat16).reshape(N_ROW, ROWS2, -1)

    def prolong_block(total, pair):
        block_pts, block_coef = pair
        kernel = wendland(block_pts, points1, support_coarse)
        return (total + jnp.dot(kernel.T, block_coef, preferred_element_type=jnp.float32), None)
    mid_corr, unused = lax.scan(prolong_block, jnp.zeros((N1, FIELDS), jnp.float32), (coarse_blocks, coarse_low))
    mid_coef = 0.5 * mid_data + scale_e2 * mid_corr
    fine_coef = 0.5 * fine_data + scale_e1 * listed_all(points0, points1, tiles_e1, mid_coef.astype(jnp.bfloat16), support_mid, False)
    norms = jnp.stack([jnp.mean(fine_res * fine_res)])
    return (fine_coef, mid_coef, coarse_coef, norms)
```

```python
import functools
import math

import jax
import jax.numpy as jnp
from jax import lax
from jax.experimental import pallas as pl
from jax.experimental.pallas import tpu as pltpu
from jax.sharding import PartitionSpec as P

TILE = 128


support_fine = 0.35
support_mid = 0.55
support_coarse = 0.8


def spread(x, axis, root):
    mine = lax.axis_index(axis) == root
    return lax.psum(jnp.where(mine, x, jnp.zeros_like(x)), axis)


def wendland(left_pts, right_pts, support):
    left = left_pts.astype(jnp.float32)
    right = right_pts.astype(jnp.float32)
    across = left[0][..., :, None] - right[0][..., None, :]
    upward = left[1][..., :, None] - right[1][..., None, :]
    ratio_t = jnp.sqrt(across * across + upward * upward) / support
    margin = jnp.maximum(1.0 - ratio_t, 0.0)
    squared = margin * margin
    return (squared * squared * (4.0 * ratio_t + 1.0)).astype(jnp.bfloat16)


def listed_terms(row_pts, col_pts, listing, vector, support, flipped):
    row_tiles = row_pts.reshape(2, -1, TILE)
    col_tiles = col_pts.reshape(2, -1, TILE)
    listed = listing.shape[-1]
    group = math.gcd(listed, 32)
    order = listing.reshape(2, listed // group, group)
    fields = vector.shape[-1]
    inputs = vector.reshape(-1, TILE, fields)
    target = col_tiles.shape[1] if flipped else row_tiles.shape[1]
    total = jnp.zeros((target, TILE, fields), jnp.float32)

    def add_group(total, pair):
        tile_rows, tile_cols = pair
        kernel = wendland(row_tiles[:, tile_rows], col_tiles[:, tile_cols], support)
        if flipped:
            contrib = jnp.einsum(
                "gij,gir->gjr", kernel, inputs[tile_rows], preferred_element_type=jnp.float32
            )
            return (total.at[tile_cols].add(contrib), None)
        contrib = jnp.einsum(
            "gij,gjr->gir", kernel, inputs[tile_cols], preferred_element_type=jnp.float32
        )
        return (total.at[tile_rows].add(contrib), None)

    total, unused = lax.scan(add_group, total, (order[0], order[1]))
    return total.reshape(-1, fields)


def per_device(values, points0, points1, points2, tiles_a0, tiles_e1, tiles_a1, factor):
    row_count = lax.axis_size("row")
    col_count = lax.axis_size("col")
    col_id = lax.axis_index("col")
    col_per_row = col_count // row_count
    rows_fine, fields = values.shape
    rows_mid = points1.shape[1]
    share = rows_fine // col_count
    cols_fine = rows_fine // col_per_row
    cols_mid = rows_mid // col_per_row
    source = col_id // col_per_row
    part_index = col_id % col_per_row
    value_piece = lax.dynamic_slice_in_dim(values, part_index * cols_fine, cols_fine, 0)
    fine_piece = lax.dynamic_slice_in_dim(points0, part_index * cols_fine, cols_fine, 1)
    mid_piece = lax.dynamic_slice_in_dim(points1, part_index * cols_mid, cols_mid, 1)
    value_cols, fine_cols, mid_cols = (
        spread(value_piece, "row", source),
        spread(fine_piece, "row", source),
        spread(mid_piece, "row", source),
    )
    scale_a0 = (rows_fine / (col_count * tiles_a0.shape[-1] * TILE * TILE)) ** 0.5
    scale_e1 = (rows_fine / (col_count * tiles_e1.shape[-1] * TILE * TILE)) ** 0.5
    scale_a1 = (rows_mid / (col_count * tiles_a1.shape[-1] * TILE * TILE)) ** 0.5
    scale_e2 = (1.0 / (rows_mid * row_count)) ** 0.5
    fine_data = values.astype(jnp.float32)
    own_data = lax.dynamic_slice_in_dim(values, col_id * share, share, 0).astype(jnp.float32)
    product_part = listed_terms(points0, fine_cols, tiles_a0[0, 0], value_cols, support_fine, False)
    product_whole = lax.psum(product_part, "col")
    fine_residual = fine_data - 0.5 * (scale_a0 * product_whole)
    fine_square = jnp.sum(fine_residual * fine_residual)
    restrict_part = listed_terms(
        points0, mid_cols, tiles_e1[0, 0], fine_residual.astype(jnp.bfloat16), support_mid, True
    )
    restrict_sum = lax.psum(restrict_part, "row")
    mid_data = scale_e1 * restrict_sum
    mid_part = listed_terms(
        points1, mid_cols, tiles_a1[0, 0], mid_data.astype(jnp.bfloat16), support_mid, False
    )
    mid_whole = (scale_a1 * lax.psum(mid_part, "col")).astype(jnp.bfloat16)
    mid_slice = lax.dynamic_slice_in_dim(mid_whole, part_index * cols_mid, cols_mid, 0)
    mid_turned = spread(mid_slice, "row", source)
    mid_residual = mid_data - 0.5 * mid_turned.astype(jnp.float32)
    coarse_kernel = wendland(points2, mid_cols, support_coarse)
    coarse_part = jnp.dot(
        coarse_kernel, mid_residual.astype(jnp.bfloat16), preferred_element_type=jnp.float32
    )
    coarse_sum = lax.psum(coarse_part, "col")
    coarse_data = (scale_e2 * coarse_sum).astype(jnp.bfloat16)
    halfway_part = lax.dot_general(
        factor, coarse_data, (((0,), (0,)), ((), ())), preferred_element_type=jnp.float32
    )
    halfway = lax.psum(halfway_part, "row").astype(jnp.bfloat16)
    coarse_part_two = jnp.dot(factor, halfway, preferred_element_type=jnp.float32)
    coarse_coef = lax.psum(coarse_part_two, "col")
    prolong_part = lax.dot_general(
        coarse_kernel,
        coarse_coef.astype(jnp.bfloat16),
        (((0,), (0,)), ((), ())),
        preferred_element_type=jnp.float32,
    )
    mid_coef = 0.5 * mid_data + scale_e2 * lax.psum(prolong_part, "row")
    fine_part = listed_terms(
        points0, mid_cols, tiles_e1[0, 0], mid_coef.astype(jnp.bfloat16), support_mid, False
    )
    fine_coef = 0.5 * own_data + scale_e1 * lax.psum_scatter(
        fine_part, "col", scatter_dimension=0, tiled=True
    )
    fine_total = lax.psum(fine_square / col_count, ("row", "col"))
    fine_norm = fine_total / (rows_fine * row_count * fields)
    return (fine_coef, mid_coef, coarse_coef, jnp.stack([fine_norm]))


FAR = 1024.0
CHUNKS = 4
MESH = pl.DeviceIdType.MESH


def phi_tile(cx, cy, rx, ry, inv_square):
    across = cx - rx
    upward = cy - ry
    square = (across * across + upward * upward) * inv_square
    t = square * lax.rsqrt(jnp.maximum(square, 1e-30))
    margin = jnp.maximum(1.0 - t, 0.0)
    squared = margin * margin
    return (squared * squared * (4.0 * t + 1.0)).astype(jnp.bfloat16)


def dot(a, b):
    return jnp.dot(a, b, preferred_element_type=jnp.float32)


def cycle_kernel(g, vals, pts, offs, fac, offe, offa, fine_o, mid_o, coarse_o, norm_o,
                 ptsg, offg, facg, vall, a0, e1own, e1t, e2t, e2c, a1, cf, cm, cc2, resg, part_buf,
                 rsin, midc, mida, rhs, csend, crecv, cg, gall, gt, ccoef, mcb,
                 p_s, p_r, o_s, o_r, f_s, f_r, vy_s, vy_r, vx_s, vx_r, vf_s, vf_r, vg_s, vg_r, vp_s, vp_r,
                 g_s, g_r, res_s, res_r, rs_s, rs_r, mc_s, mc_r, mq_s, mq_r, mf_s, mf_r, cr_s, cr_r, ca_s, ca_r):
    nr, nc, R0, R1, R2 = g["nr"], g["nc"], g["R0"], g["R1"], g["R2"]
    D = nr * nc
    T0, T1 = R0 // TILE, R1 // TILE
    C0, C1 = R0 * nr // nc, R1 * nr // nc
    B0, B1 = C0 // TILE, C1 // TILE
    S0 = R0 // nc
    I0 = S0 // TILE
    Q1 = C1 // nr
    CR = R2 * nr // D
    NT1 = nr * T1
    NT2 = nr * R2 // TILE
    X1, Y1, X2 = 2 * T0, 2 * T0 + T1, 2 * T0 + 2 * T1
    fine_inv, mid_inv, coarse_inv = (1.0 / (s * s) for s in (support_fine, support_mid, support_coarse))
    r = lax.axis_index("row")
    c = lax.axis_index("col")
    d = r * nc + c
    mate = r + 1 - 2 * lax.rem(r, 2)
    yp = lax.rem(r + 2, nr)
    diag = lax.rem(mate + 2, nr)
    h = lax.rem(c, 2)
    xp = c + 1 - 2 * h

    def rc(src, dst, ssem, rsem, rr, cc):
        return pltpu.make_async_remote_copy(src_ref=src, dst_ref=dst, send_sem=ssem, recv_sem=rsem,
                                            device_id=(rr, cc), device_id_type=MESH)

    def each(lo, hi, f):
        def body(k, carry):
            f(k)
            return carry
        lax.fori_loop(lo, hi, body, 0)

    barrier = pltpu.get_barrier_semaphore()

    def greet(k):
        peer = lax.rem(d + k, D)
        pl.semaphore_signal(barrier, inc=1, device_id=(peer // nc, lax.rem(peer, nc)), device_id_type=MESH)

    each(1, D, greet)
    pl.semaphore_wait(barrier, D - 1)

    def row_send(src_of, dst, ss, rr):
        for k in range(1, nr):
            q = lax.rem(r + k, nr)
            rc(src_of(q), dst, ss.at[k], rr.at[r], q, c).start()

    def row_wait(src, dst_of, ss, rr):
        for k in range(1, nr):
            q = lax.rem(r + k, nr)
            rc(src, dst_of(q), ss.at[k], rr.at[q], q, c).wait()

    def col_send(src_of, dst, ss, rr):
        def go(k):
            q = lax.rem(c + k, nc)
            rc(src_of(q), dst, ss.at[k], rr.at[c], r, q).start()
        each(1, nc, go)

    def col_wait(src, dst_of, ss, rr):
        def go(k):
            q = lax.rem(c + k, nc)
            rc(src, dst_of(q), ss.at[k], rr.at[q], r, q).wait()
        each(1, nc, go)

    row_send(lambda q: pts, ptsg.at[r], p_s, p_r)
    HALF = R0 // 2
    CH = HALF // CHUNKS

    def chunk(half, q):
        return pl.ds(pl.multiple_of(half * HALF + q * CH, CH), CH)

    def y_copy(q):
        return rc(vals.at[chunk(h, q)], vall.at[r, chunk(h, q)], vy_s.at[q], vy_r.at[q], yp, c)

    def y_in(q):
        return rc(vals.at[chunk(h, q)], vall.at[yp, chunk(h, q)], vy_s.at[q], vy_r.at[q], yp, c)

    def x_copy(q):
        return rc(vall.at[yp, chunk(h, q)], vall.at[yp, chunk(h, q)], vx_s.at[q], vx_r.at[q], r, xp)

    def x_in(q):
        return rc(vall.at[yp, chunk(h, q)], vall.at[yp, chunk(1 - h, q)], vx_s.at[q], vx_r.at[q], r, xp)

    def f_copy(q):
        return rc(vall.at[yp, chunk(h, q)], vall.at[yp, chunk(h, q)], vf_s.at[q], vf_r.at[q], mate, c)

    def f_in(q):
        return rc(vall.at[yp, chunk(h, q)], vall.at[diag, chunk(h, q)], vf_s.at[q], vf_r.at[q], mate, c)

    def g_copy(q):
        return rc(vall.at[yp, chunk(1 - h, q)], vall.at[yp, chunk(1 - h, q)], vg_s.at[q], vg_r.at[q], mate, c)

    def g_in(q):
        return rc(vall.at[yp, chunk(1 - h, q)], vall.at[diag, chunk(1 - h, q)], vg_s.at[q], vg_r.at[q], mate, c)

    for q in range(CHUNKS):
        y_copy(q).start()
    col_send(lambda q: offs.at[q], offg.at[c], o_s, o_r)
    mate_copy = rc(vals, vall.at[r], vp_s.at[0], vp_r.at[0], mate, c)
    mate_copy.start()
    col_send(lambda q: fac, facg.at[c], f_s, f_r)
    ptsg[r] = pts[...]
    offg[c] = offs[c]
    facg[c] = fac[...]

    def turned(row):
        return jnp.broadcast_to(row, (TILE, TILE)).T

    for i in range(I0):
        for way in range(2):
            cf[2 * i + way] = turned(pts[pl.ds(way * T0 + c * I0 + i, 1), :])
    row_wait(pts, lambda q: ptsg.at[q], p_s, p_r)
    col_wait(offs.at[0], lambda q: offg.at[q], o_s, o_r)

    blocks = (r, mate, yp, diag)
    for s, rb in enumerate(blocks):
        def build_a0(kk, s=s, rb=rb):
            rx = ptsg[rb, pl.ds(kk, 1), :]
            ry = ptsg[rb, pl.ds(T0 + kk, 1), :]
            cb = rb * (nc // nr) + kk // B0
            j = lax.rem(kk, B0)
            for i in range(I0):
                off = offg[cb, pl.ds(i * B0 + j, 1), :]
                a0[s, i * TILE:(i + 1) * TILE, pl.ds(pl.multiple_of(kk * TILE, TILE), TILE)] = phi_tile(
                    cf[2 * i], cf[2 * i + 1], rx + off, ry, fine_inv)
        each(0, T0, build_a0)
        if s < CHUNKS:
            y_in(s).wait_recv()
            x_copy(s).start()
            f_copy(s).start()
    acc = dot(a0[0], vals[...])
    for q in range(CHUNKS):
        x_in(q).wait_recv()
        g_copy(q).start()
    rc(vals, vall.at[mate], vp_s.at[0], vp_r.at[0], mate, c).wait_recv()
    acc = acc + dot(a0[1], vall[mate])
    acc = acc + dot(a0[2], vall[yp])
    for q in range(CHUNKS):
        f_in(q).wait_recv()
        g_in(q).wait_recv()
    acc = acc + dot(a0[3], vall[diag])
    own_vals = vals[pl.ds(pl.multiple_of(c * S0, S0), S0), :].astype(jnp.float32)
    res = own_vals - (0.5 * g["scale_a0"]) * acc
    square = jnp.sum((res * res).reshape(S0 // 8, 8, -1), axis=0)

    def res_at(q):
        return resg.at[pl.ds(pl.multiple_of(q * S0, S0), S0)]

    resg[pl.ds(pl.multiple_of(c * S0, S0), S0), :] = res.astype(jnp.bfloat16)
    col_send(lambda q: res_at(c), res_at(c), res_s, res_r)

    def turn_mid(k):
        for way in range(2):
            cm[k, way] = turned(ptsg[k // T1, pl.ds(X1 + way * T1 + lax.rem(k, T1), 1), :])
    each(0, NT1, turn_mid)

    def build_e1t(i):
        rx, ry = pts[pl.ds(i, 1), :], pts[pl.ds(T0 + i, 1), :]
        for j in range(B1):
            off = offe[pl.ds(j * T0 + i, 1), :]
            e1t[j * TILE:(j + 1) * TILE, pl.ds(pl.multiple_of(i * TILE, TILE), TILE)] = phi_tile(
                cm[c * B1 + j, 0], cm[c * B1 + j, 1], rx + off, ry, mid_inv)
    each(0, T0, build_e1t)
    col_wait(fac, lambda q: facg.at[q], f_s, f_r)
    per_lane = nc * TILE // g["N2"]
    for lane in range(g["N2"] // TILE):
        total = facg[lane * per_lane].astype(jnp.float32)
        for k in range(1, per_lane):
            total = total + facg[lane * per_lane + k].astype(jnp.float32)
        gall[r, :, lane * TILE:(lane + 1) * TILE] = total.astype(jnp.bfloat16)
    row_send(lambda q: gall.at[r], gall.at[r], g_s, g_r)

    def coarse_row(t, way):
        per = TILE // R2
        return ptsg[per * t, X2 + way:X2 + way + 1, :] + ptsg[per * t + 1, X2 + 2 + way:X2 + 3 + way, :]

    for i in range(T1):
        for j in range(B1):
            mt = c * B1 + j
            rx = ptsg[mt // T1, pl.ds(X1 + lax.rem(mt, T1), 1), :]
            ry = ptsg[mt // T1, pl.ds(Y1 + lax.rem(mt, T1), 1), :]
            off = offa[i * B1 + j:i * B1 + j + 1, :]
            a1[i * TILE:(i + 1) * TILE, j * TILE:(j + 1) * TILE] = phi_tile(
                cm[r * T1 + i, 0], cm[r * T1 + i, 1], rx + off, ry, mid_inv)
    for t in range(NT2):
        for way in range(2):
            cc2[2 * t + way] = turned(coarse_row(t, way))

    def build_e2c(k):
        mt = jnp.where(k < T1, r * T1 + k, c * B1 + k - T1)
        rx = ptsg[mt // T1, pl.ds(X1 + lax.rem(mt, T1), 1), :]
        ry = ptsg[mt // T1, pl.ds(Y1 + lax.rem(mt, T1), 1), :]
        for t in range(NT2):
            e2c[t * TILE:(t + 1) * TILE, pl.ds(pl.multiple_of(k * TILE, TILE), TILE)] = phi_tile(
                cc2[2 * t], cc2[2 * t + 1], rx, ry, coarse_inv)
    each(0, T1 + B1, build_e2c)

    def build_e1own(k):
        rx = ptsg[k // T1, pl.ds(X1 + lax.rem(k, T1), 1), :]
        ry = ptsg[k // T1, pl.ds(Y1 + lax.rem(k, T1), 1), :]
        for i in range(I0):
            off = offg[k // B1, pl.ds(I0 * B0 + i * B1 + lax.rem(k, B1), 1), :]
            e1own[i * TILE:(i + 1) * TILE, pl.ds(pl.multiple_of(k * TILE, TILE), TILE)] = phi_tile(
                cf[2 * i], cf[2 * i + 1], rx + off, ry, mid_inv)
    each(0, NT1, build_e1own)

    def build_e2t(k):
        for t in range(NT2):
            e2t[pl.ds(pl.multiple_of(k * TILE, TILE), TILE), t * TILE:(t + 1) * TILE] = phi_tile(
                cm[k, 0], cm[k, 1], coarse_row(t, 0), coarse_row(t, 1), coarse_inv)
    each(0, NT1, build_e2t)
    row_wait(gall.at[r], lambda q: gall.at[q], g_s, g_r)
    whole = gall[...].reshape(g["N2"], g["N2"])
    gt[...] = whole.astype(jnp.float32).T.astype(jnp.bfloat16)

    col_wait(res_at(c), res_at, res_s, res_r)
    part_buf[...] = dot(e1t[...], resg[...]).reshape(nr, Q1, -1)
    row_send(lambda q: part_buf.at[q], rsin.at[r], rs_s, rs_r)
    rsin[r] = part_buf[r]
    row_wait(part_buf.at[0], lambda q: rsin.at[q], rs_s, rs_r)
    quarter = rsin[0]
    for k in range(1, nr):
        quarter = quarter + rsin[k]
    quarter = g["scale_e1"] * quarter
    midc[r] = quarter
    mida[r, c] = quarter.astype(jnp.bfloat16)
    row_send(lambda q: midc.at[r], midc.at[r], mc_s, mc_r)
    col_send(lambda q: mida.at[r, c], mida.at[r, c], mq_s, mq_r)
    row_wait(midc.at[r], lambda q: midc.at[q], mc_s, mc_r)
    mid_col = midc[...].reshape(C1, -1).astype(jnp.bfloat16)
    rhs[:R1] = ((-0.5 * g["scale_a1"]) * dot(a1[...], mid_col)).astype(jnp.bfloat16)
    for k in range(nr):
        rhs[R1 + k * Q1:R1 + (k + 1) * Q1] = jnp.where(r == k, midc[k], 0.0).astype(jnp.bfloat16)
    csend[:, :CR] = (g["scale_e2"] * dot(e2c[...], rhs[...])).reshape(D, CR, -1)
    csend[:, CR:] = jnp.broadcast_to(square[None], (D,) + square.shape)

    def cr_go(k):
        peer = lax.rem(d + k, D)
        rc(csend.at[peer], crecv.at[d], cr_s.at[k], cr_r.at[d], peer // nc, lax.rem(peer, nc)).start()
    each(1, D, cr_go)
    crecv[d] = csend[d]
    col_wait(mida.at[r, c], lambda q: mida.at[r, q], mq_s, mq_r)
    def cr_wait(k):
        peer = lax.rem(d + k, D)
        rc(csend.at[peer], crecv.at[peer], cr_s.at[k], cr_r.at[peer], peer // nc, lax.rem(peer, nc)).wait()
    each(1, D, cr_wait)
    sums = jnp.sum(crecv[...], axis=0)

    def cg_at(q):
        return cg.at[pl.ds(pl.multiple_of(q * CR, CR), CR)]

    cg[pl.ds(pl.multiple_of(d * CR, CR), CR), :] = sums[:CR]

    def ca_go(k):
        peer = lax.rem(d + k, D)
        rc(cg_at(d), cg_at(d), ca_s.at[k], ca_r.at[d], peer // nc, lax.rem(peer, nc)).start()
    each(1, D, ca_go)
    row_send(lambda q: mida.at[r], mida.at[r], mf_s, mf_r)
    norm_o[...] = jnp.broadcast_to(jnp.sum(sums[CR:], keepdims=True) * g["norm_scale"], norm_o.shape)
    def ca_wait(k):
        peer = lax.rem(d + k, D)
        rc(cg_at(d), cg_at(peer), ca_s.at[k], ca_r.at[peer], peer // nc, lax.rem(peer, nc)).wait()
    each(1, D, ca_wait)
    halfway = dot(gt[...], cg[...].astype(jnp.bfloat16)).astype(jnp.bfloat16)
    ccoef[...] = dot(gall[...].reshape(g["N2"], g["N2"]), halfway)
    coarse_o[...] = ccoef[pl.ds(pl.multiple_of(r * R2, R2), R2), :]
    coarse_low = ccoef[...].astype(jnp.bfloat16)
    own_rows = pl.ds(pl.multiple_of(c * C1, C1), C1)
    mid_o[...] = 0.5 * midc[...].reshape(C1, -1) + g["scale_e2"] * dot(e2t[own_rows, :], coarse_low)
    row_wait(mida.at[r], lambda q: mida.at[q], mf_s, mf_r)
    for q in range(nc):
        corr = g["scale_e2"] * dot(e2t[q * C1:(q + 1) * C1, :], coarse_low)
        for k in range(nr):
            mcb[q * C1 + k * Q1:q * C1 + (k + 1) * Q1] = (
                0.5 * mida[k, q].astype(jnp.float32) + corr[k * Q1:(k + 1) * Q1]).astype(jnp.bfloat16)
    fine_o[...] = 0.5 * own_vals + g["scale_e1"] * dot(e1own[...], mcb[...])
    for q in range(CHUNKS):
        y_copy(q).wait_send()
        x_copy(q).wait_send()
        f_copy(q).wait_send()
        g_copy(q).wait_send()
    mate_copy.wait_send()


def far_of(listing, row_tiles, col_tiles):
    key = listing[0] * col_tiles + listing[1]
    hit = jnp.any(jnp.arange(row_tiles * col_tiles)[:, None] == key[None, :], axis=1)
    return jnp.where(hit, 0.0, FAR).astype(jnp.float32).reshape(row_tiles, col_tiles)


def fits(nr, nc, R0, R1, R2):
    if nr != 4 or nc % nr or (nc // nr) % 2:
        return False
    if R0 % (nc * TILE) or (R1 * nr) % (nc * TILE) or R1 % TILE or 2 * R2 != TILE:
        return False
    if (nr * R2) % (nr * nc * 8) or (nr * R2) % TILE or (nc * TILE) % (nr * R2):
        return False
    return 2 * (R0 // nc) * R0 * nr <= 8 << 20


def fused(values, points0, points1, points2, tiles_a0, tiles_e1, tiles_a1, factor):
    nr, nc = lax.axis_size("row"), lax.axis_size("col")
    R0, R1, R2 = points0.shape[1], points1.shape[1], points2.shape[1]
    F = values.shape[-1]
    if not fits(nr, nc, R0, R1, R2) or F != TILE:
        return per_device(values, points0, points1, points2, tiles_a0, tiles_e1, tiles_a1, factor)
    c = lax.axis_index("col")
    D, N2 = nr * nc, nr * R2
    T0, T1 = R0 // TILE, R1 // TILE
    B0, B1 = R0 * nr // nc // TILE, R1 * nr // nc // TILE
    S0 = R0 // nc
    I0 = S0 // TILE
    C1, CR, Q1 = B1 * TILE, N2 // D, R1 // nc
    p0, p1, p2 = (p.astype(jnp.float32) for p in (points0, points1, points2))
    rows = [p0.reshape(2 * T0, TILE), p1.reshape(2 * T1, TILE),
            jnp.pad(p2, ((0, 0), (0, TILE - R2))), jnp.pad(p2, ((0, 0), (TILE - R2, 0)))]
    used = 2 * T0 + 2 * T1 + 4
    NP = -(-used // 8) * 8
    pts = jnp.pad(jnp.concatenate(rows, axis=0), ((0, NP - used), (0, 0)))
    far_a0 = far_of(tiles_a0[0, 0], T0, B0)
    far_e1 = far_of(tiles_e1[0, 0], T0, B1)
    far_a1 = far_of(tiles_a1[0, 0], T1, B1)
    NO = I0 * (B0 + B1)
    NOP = -(-NO // 8) * 8
    per_peer = jnp.concatenate([far_a0.reshape(nc, I0 * B0), far_e1.reshape(nc, I0 * B1)], axis=1)
    per_peer = jnp.pad(per_peer, ((0, 0), (0, NOP - NO)))
    offs = jnp.broadcast_to(per_peer[:, :, None], (nc, NOP, TILE))
    offe = jnp.broadcast_to(far_e1.T.reshape(-1, 1), (B1 * T0, TILE))
    offa = jnp.broadcast_to(far_a1.reshape(-1, 1), (T1 * B1, TILE))
    width = factor.shape[1]
    fac = lax.dynamic_update_slice(jnp.zeros((R2, TILE), factor.dtype), factor, (0, lax.rem(c, TILE // width) * width))
    g = dict(nr=nr, nc=nc, R0=R0, R1=R1, R2=R2, N2=N2,
             scale_a0=(R0 / (nc * tiles_a0.shape[-1] * TILE * TILE)) ** 0.5,
             scale_e1=(R0 / (nc * tiles_e1.shape[-1] * TILE * TILE)) ** 0.5,
             scale_a1=(R1 / (nc * tiles_a1.shape[-1] * TILE * TILE)) ** 0.5,
             scale_e2=(1.0 / (R1 * nr)) ** 0.5,
             norm_scale=1.0 / (R0 * nr * F))
    f32, bf16 = jnp.float32, jnp.bfloat16
    V = pltpu.VMEM
    dma = pltpu.SemaphoreType.DMA
    scratch = [
        V((nr, NP, TILE), f32), V((nc, NOP, TILE), f32), V((nc, R2, TILE), bf16),
        V((nr, R0, F), bf16), V((nr, S0, R0), bf16), V((S0, nr * R1), bf16), V((C1, R0), bf16),
        V((nr * R1, N2), bf16), V((N2, R1 + C1), bf16), V((R1, C1), bf16),
        V((2 * I0, TILE, TILE), f32), V((nr * T1, 2, TILE, TILE), f32), V((2 * N2 // TILE, TILE, TILE), f32),
        V((R0, F), bf16), V((nr, Q1, F), f32), V((nr, Q1, F), f32), V((nr, Q1, F), f32),
        V((nr, nc, Q1, F), bf16), V((R1 + C1, F), bf16), V((D, CR + 8, F), f32), V((D, CR + 8, F), f32),
        V((N2, F), f32), V((nr, R2, N2), bf16), V((N2, N2), bf16), V((N2, F), f32), V((nr * R1, F), bf16),
    ]
    for n in (nr, nc, nc, CHUNKS, CHUNKS, CHUNKS, CHUNKS, 1, nr, nc, nr, nr, nc, nr, D, D):
        scratch += [dma((n,)), dma((n,))]
    vm = pl.BlockSpec(memory_space=pltpu.VMEM)
    fine, mid, coarse, norm = pl.pallas_call(
        functools.partial(cycle_kernel, g),
        out_shape=(jax.ShapeDtypeStruct((S0, F), f32), jax.ShapeDtypeStruct((C1, F), f32),
                   jax.ShapeDtypeStruct((R2, F), f32), jax.ShapeDtypeStruct((8, TILE), f32)),
        in_specs=[vm] * 6,
        out_specs=[vm] * 4,
        scratch_shapes=scratch,
        compiler_params=pltpu.CompilerParams(collective_id=0, has_side_effects=True, vmem_limit_bytes=48 << 20),
    )(values, pts, offs, fac, offe, offa)
    return (fine, mid, coarse, norm[0, :1])


def solution(mesh):
    return jax.shard_map(
        fused,
        mesh=mesh,
        in_specs=(
            P("row", None),
            P(None, "row"),
            P(None, "row"),
            P(None, "row"),
            P("row", "col", None, None),
            P("row", "col", None, None),
            P("row", "col", None, None),
            P("row", "col"),
        ),
        out_specs=(P(("row", "col"), None), P("col", None), P("row", None), P()),
        check_vma=False,
    )
```

```python
import functools
import math

import jax
import jax.numpy as jnp
from jax import lax
from jax.experimental import pallas as pl
from jax.experimental.pallas import tpu as pltpu
from jax.sharding import PartitionSpec as P

TILE = 128


support_fine = 0.35
support_mid = 0.55
support_coarse = 0.8


def spread(x, axis, root):
    mine = lax.axis_index(axis) == root
    return lax.psum(jnp.where(mine, x, jnp.zeros_like(x)), axis)


def wendland(left_pts, right_pts, support):
    left = left_pts.astype(jnp.float32)
    right = right_pts.astype(jnp.float32)
    across = left[0][..., :, None] - right[0][..., None, :]
    upward = left[1][..., :, None] - right[1][..., None, :]
    ratio_t = jnp.sqrt(across * across + upward * upward) / support
    margin = jnp.maximum(1.0 - ratio_t, 0.0)
    squared = margin * margin
    return (squared * squared * (4.0 * ratio_t + 1.0)).astype(jnp.bfloat16)


def listed_terms(row_pts, col_pts, listing, vector, support, flipped):
    row_tiles = row_pts.reshape(2, -1, TILE)
    col_tiles = col_pts.reshape(2, -1, TILE)
    listed = listing.shape[-1]
    group = math.gcd(listed, 32)
    order = listing.reshape(2, listed // group, group)
    fields = vector.shape[-1]
    inputs = vector.reshape(-1, TILE, fields)
    target = col_tiles.shape[1] if flipped else row_tiles.shape[1]
    total = jnp.zeros((target, TILE, fields), jnp.float32)

    def add_group(total, pair):
        tile_rows, tile_cols = pair
        kernel = wendland(row_tiles[:, tile_rows], col_tiles[:, tile_cols], support)
        if flipped:
            contrib = jnp.einsum(
                "gij,gir->gjr", kernel, inputs[tile_rows], preferred_element_type=jnp.float32
            )
            return (total.at[tile_cols].add(contrib), None)
        contrib = jnp.einsum(
            "gij,gjr->gir", kernel, inputs[tile_cols], preferred_element_type=jnp.float32
        )
        return (total.at[tile_rows].add(contrib), None)

    total, unused = lax.scan(add_group, total, (order[0], order[1]))
    return total.reshape(-1, fields)


def per_device(values, points0, points1, points2, tiles_a0, tiles_e1, tiles_a1, factor):
    row_count = lax.axis_size("row")
    col_count = lax.axis_size("col")
    col_id = lax.axis_index("col")
    col_per_row = col_count // row_count
    rows_fine, fields = values.shape
    rows_mid = points1.shape[1]
    share = rows_fine // col_count
    cols_fine = rows_fine // col_per_row
    cols_mid = rows_mid // col_per_row
    source = col_id // col_per_row
    part_index = col_id % col_per_row
    value_piece = lax.dynamic_slice_in_dim(values, part_index * cols_fine, cols_fine, 0)
    fine_piece = lax.dynamic_slice_in_dim(points0, part_index * cols_fine, cols_fine, 1)
    mid_piece = lax.dynamic_slice_in_dim(points1, part_index * cols_mid, cols_mid, 1)
    value_cols, fine_cols, mid_cols = (
        spread(value_piece, "row", source),
        spread(fine_piece, "row", source),
        spread(mid_piece, "row", source),
    )
    scale_a0 = (rows_fine / (col_count * tiles_a0.shape[-1] * TILE * TILE)) ** 0.5
    scale_e1 = (rows_fine / (col_count * tiles_e1.shape[-1] * TILE * TILE)) ** 0.5
    scale_a1 = (rows_mid / (col_count * tiles_a1.shape[-1] * TILE * TILE)) ** 0.5
    scale_e2 = (1.0 / (rows_mid * row_count)) ** 0.5
    fine_data = values.astype(jnp.float32)
    own_data = lax.dynamic_slice_in_dim(values, col_id * share, share, 0).astype(jnp.float32)
    product_part = listed_terms(points0, fine_cols, tiles_a0[0, 0], value_cols, support_fine, False)
    product_whole = lax.psum(product_part, "col")
    fine_residual = fine_data - 0.5 * (scale_a0 * product_whole)
    fine_square = jnp.sum(fine_residual * fine_residual)
    restrict_part = listed_terms(
        points0, mid_cols, tiles_e1[0, 0], fine_residual.astype(jnp.bfloat16), support_mid, True
    )
    restrict_sum = lax.psum(restrict_part, "row")
    mid_data = scale_e1 * restrict_sum
    mid_part = listed_terms(
        points1, mid_cols, tiles_a1[0, 0], mid_data.astype(jnp.bfloat16), support_mid, False
    )
    mid_whole = (scale_a1 * lax.psum(mid_part, "col")).astype(jnp.bfloat16)
    mid_slice = lax.dynamic_slice_in_dim(mid_whole, part_index * cols_mid, cols_mid, 0)
    mid_turned = spread(mid_slice, "row", source)
    mid_residual = mid_data - 0.5 * mid_turned.astype(jnp.float32)
    coarse_kernel = wendland(points2, mid_cols, support_coarse)
    coarse_part = jnp.dot(
        coarse_kernel, mid_residual.astype(jnp.bfloat16), preferred_element_type=jnp.float32
    )
    coarse_sum = lax.psum(coarse_part, "col")
    coarse_data = (scale_e2 * coarse_sum).astype(jnp.bfloat16)
    halfway_part = lax.dot_general(
        factor, coarse_data, (((0,), (0,)), ((), ())), preferred_element_type=jnp.float32
    )
    halfway = lax.psum(halfway_part, "row").astype(jnp.bfloat16)
    coarse_part_two = jnp.dot(factor, halfway, preferred_element_type=jnp.float32)
    coarse_coef = lax.psum(coarse_part_two, "col")
    prolong_part = lax.dot_general(
        coarse_kernel,
        coarse_coef.astype(jnp.bfloat16),
        (((0,), (0,)), ((), ())),
        preferred_element_type=jnp.float32,
    )
    mid_coef = 0.5 * mid_data + scale_e2 * lax.psum(prolong_part, "row")
    fine_part = listed_terms(
        points0, mid_cols, tiles_e1[0, 0], mid_coef.astype(jnp.bfloat16), support_mid, False
    )
    fine_coef = 0.5 * own_data + scale_e1 * lax.psum_scatter(
        fine_part, "col", scatter_dimension=0, tiled=True
    )
    fine_total = lax.psum(fine_square / col_count, ("row", "col"))
    fine_norm = fine_total / (rows_fine * row_count * fields)
    return (fine_coef, mid_coef, coarse_coef, jnp.stack([fine_norm]))


FAR = 1024.0
CHUNKS = 4
MESH = pl.DeviceIdType.MESH


def phi_tile(cx, cy, rx, ry, inv_square):
    across = cx - rx
    upward = cy - ry
    square = (across * across + upward * upward) * inv_square
    t = square * lax.rsqrt(jnp.maximum(square, 1e-30))
    margin = jnp.maximum(1.0 - t, 0.0)
    squared = margin * margin
    return (squared * squared * (4.0 * t + 1.0)).astype(jnp.bfloat16)


def dot(a, b):
    return jnp.dot(a, b, preferred_element_type=jnp.float32)


def far_rows(tiles, row_tiles, col_tiles, by_col):
    row, col = tiles[0, 0, 0:1, :], tiles[0, 0, 1:2, :]
    key = col * row_tiles + row if by_col else row * col_tiles + col
    count = row_tiles * col_tiles
    place = lax.broadcasted_iota(jnp.int32, (count, key.shape[1]), 0)
    near = jnp.max(jnp.where(place == key, 1.0, 0.0), axis=1, keepdims=True)
    return jnp.broadcast_to(FAR * (1.0 - near), (count, TILE))


def cycle_kernel(g, vals, points0, points1, points2, tiles_a0, tiles_e1, tiles_a1, factor, fine_o, mid_o, coarse_o, norm_o,
                 pts, offs, fac, offe, offa, ptsg, offg, facg, vall, a0, e1own, e1t, e2t, e2c, a1, cf, cm, cc2, resg, part_buf,
                 rsin, midc, mida, rhs, csend, crecv, cg, gall, gt, ccoef, mcb,
                 p_s, p_r, o_s, o_r, f_s, f_r, vy_s, vy_r, vx_s, vx_r, vf_s, vf_r, vg_s, vg_r, vp_s, vp_r,
                 g_s, g_r, res_s, res_r, rs_s, rs_r, mc_s, mc_r, mq_s, mq_r, mf_s, mf_r, cr_s, cr_r, ca_s, ca_r):
    nr, nc, R0, R1, R2 = g["nr"], g["nc"], g["R0"], g["R1"], g["R2"]
    D = nr * nc
    T0, T1 = R0 // TILE, R1 // TILE
    C0, C1 = R0 * nr // nc, R1 * nr // nc
    B0, B1 = C0 // TILE, C1 // TILE
    S0 = R0 // nc
    I0 = S0 // TILE
    Q1 = C1 // nr
    CR = R2 * nr // D
    NT1 = nr * T1
    NT2 = nr * R2 // TILE
    X1, Y1, X2 = 2 * T0, 2 * T0 + T1, 2 * T0 + 2 * T1
    fine_inv, mid_inv, coarse_inv = (1.0 / (s * s) for s in (support_fine, support_mid, support_coarse))
    r = lax.axis_index("row")
    c = lax.axis_index("col")
    d = r * nc + c
    mate = r + 1 - 2 * lax.rem(r, 2)
    yp = lax.rem(r + 2, nr)
    diag = lax.rem(mate + 2, nr)
    h = lax.rem(c, 2)
    xp = c + 1 - 2 * h

    def rc(src, dst, ssem, rsem, rr, cc):
        return pltpu.make_async_remote_copy(src_ref=src, dst_ref=dst, send_sem=ssem, recv_sem=rsem,
                                            device_id=(rr, cc), device_id_type=MESH)

    def each(lo, hi, f):
        def body(k, carry):
            f(k)
            return carry
        lax.fori_loop(lo, hi, body, 0)

    barrier = pltpu.get_barrier_semaphore()

    def greet(k):
        peer = lax.rem(d + k, D)
        pl.semaphore_signal(barrier, inc=1, device_id=(peer // nc, lax.rem(peer, nc)), device_id_type=MESH)

    each(1, D, greet)
    pl.semaphore_wait(barrier, D - 1)

    pts[...] = jnp.zeros_like(pts)
    for way in range(2):
        for ref, at, count in ((points0, way * T0, T0), (points1, X1 + way * T1, T1)):
            line = ref[way:way + 1, :].astype(jnp.float32)
            for k in range(count):
                pts[at + k:at + k + 1, :] = line[:, k * TILE:(k + 1) * TILE]
        line = points2[way:way + 1, :].astype(jnp.float32)
        blank = jnp.zeros((1, TILE - R2), jnp.float32)
        pts[X2 + way:X2 + way + 1, :] = jnp.concatenate([line, blank], axis=1)
        pts[X2 + 2 + way:X2 + 3 + way, :] = jnp.concatenate([blank, line], axis=1)

    def row_send(src_of, dst, ss, rr):
        for k in range(1, nr):
            q = lax.rem(r + k, nr)
            rc(src_of(q), dst, ss.at[k], rr.at[r], q, c).start()

    def row_wait(src, dst_of, ss, rr):
        for k in range(1, nr):
            q = lax.rem(r + k, nr)
            rc(src, dst_of(q), ss.at[k], rr.at[q], q, c).wait()

    def col_send(src_of, dst, ss, rr):
        def go(k):
            q = lax.rem(c + k, nc)
            rc(src_of(q), dst, ss.at[k], rr.at[c], r, q).start()
        each(1, nc, go)

    def col_wait(src, dst_of, ss, rr):
        def go(k):
            q = lax.rem(c + k, nc)
            rc(src, dst_of(q), ss.at[k], rr.at[q], r, q).wait()
        each(1, nc, go)

    far_a0 = far_rows(tiles_a0, T0, B0, False)
    far_e1 = far_rows(tiles_e1, T0, B1, False)
    offs[...] = jnp.zeros_like(offs)
    for q in range(nc):
        offs[q, :I0 * B0] = far_a0[q * I0 * B0:(q + 1) * I0 * B0]
        offs[q, I0 * B0:I0 * (B0 + B1)] = far_e1[q * I0 * B1:(q + 1) * I0 * B1]
    wide = factor.shape[1]
    lane_of = lax.rem(c, TILE // wide)
    raw = factor[...].astype(jnp.float32)
    fac[...] = jnp.concatenate([jnp.where(lane_of == k, raw, 0.0) for k in range(TILE // wide)], axis=1).astype(jnp.bfloat16)
    row_send(lambda q: pts, ptsg.at[r], p_s, p_r)
    HALF = R0 // 2
    CH = HALF // CHUNKS

    def chunk(half, q):
        return pl.ds(pl.multiple_of(half * HALF + q * CH, CH), CH)

    def y_copy(q):
        return rc(vals.at[chunk(h, q)], vall.at[r, chunk(h, q)], vy_s.at[q], vy_r.at[q], yp, c)

    def y_in(q):
        return rc(vals.at[chunk(h, q)], vall.at[yp, chunk(h, q)], vy_s.at[q], vy_r.at[q], yp, c)

    def x_copy(q):
        return rc(vall.at[yp, chunk(h, q)], vall.at[yp, chunk(h, q)], vx_s.at[q], vx_r.at[q], r, xp)

    def x_in(q):
        return rc(vall.at[yp, chunk(h, q)], vall.at[yp, chunk(1 - h, q)], vx_s.at[q], vx_r.at[q], r, xp)

    def f_copy(q):
        return rc(vall.at[yp, chunk(h, q)], vall.at[yp, chunk(h, q)], vf_s.at[q], vf_r.at[q], mate, c)

    def f_in(q):
        return rc(vall.at[yp, chunk(h, q)], vall.at[diag, chunk(h, q)], vf_s.at[q], vf_r.at[q], mate, c)

    def g_copy(q):
        return rc(vall.at[yp, chunk(1 - h, q)], vall.at[yp, chunk(1 - h, q)], vg_s.at[q], vg_r.at[q], mate, c)

    def g_in(q):
        return rc(vall.at[yp, chunk(1 - h, q)], vall.at[diag, chunk(1 - h, q)], vg_s.at[q], vg_r.at[q], mate, c)

    for q in range(CHUNKS):
        y_copy(q).start()
    col_send(lambda q: offs.at[q], offg.at[c], o_s, o_r)
    mate_copy = rc(vals, vall.at[r], vp_s.at[0], vp_r.at[0], mate, c)
    mate_copy.start()
    col_send(lambda q: fac, facg.at[c], f_s, f_r)
    ptsg[r] = pts[...]
    offg[c] = offs[c]
    facg[c] = fac[...]

    offe[...] = far_rows(tiles_e1, T0, B1, True)
    offa[...] = far_rows(tiles_a1, T1, B1, False)

    def turned(row):
        return jnp.broadcast_to(row, (TILE, TILE)).T

    for i in range(I0):
        for way in range(2):
            cf[2 * i + way] = turned(pts[pl.ds(way * T0 + c * I0 + i, 1), :])
    row_wait(pts, lambda q: ptsg.at[q], p_s, p_r)
    col_wait(offs.at[0], lambda q: offg.at[q], o_s, o_r)

    blocks = (r, mate, yp, diag)
    for s, rb in enumerate(blocks):
        def build_a0(kk, s=s, rb=rb):
            rx = ptsg[rb, pl.ds(kk, 1), :]
            ry = ptsg[rb, pl.ds(T0 + kk, 1), :]
            cb = rb * (nc // nr) + kk // B0
            j = lax.rem(kk, B0)
            for i in range(I0):
                off = offg[cb, pl.ds(i * B0 + j, 1), :]
                a0[s, i * TILE:(i + 1) * TILE, pl.ds(pl.multiple_of(kk * TILE, TILE), TILE)] = phi_tile(
                    cf[2 * i], cf[2 * i + 1], rx + off, ry, fine_inv)
        each(0, T0, build_a0)
        if s < CHUNKS:
            y_in(s).wait_recv()
            x_copy(s).start()
            f_copy(s).start()
    acc = dot(a0[0], vals[...])
    for q in range(CHUNKS):
        x_in(q).wait_recv()
        g_copy(q).start()
    rc(vals, vall.at[mate], vp_s.at[0], vp_r.at[0], mate, c).wait_recv()
    acc = acc + dot(a0[1], vall[mate])
    acc = acc + dot(a0[2], vall[yp])
    for q in range(CHUNKS):
        f_in(q).wait_recv()
        g_in(q).wait_recv()
    acc = acc + dot(a0[3], vall[diag])
    own_vals = vals[pl.ds(pl.multiple_of(c * S0, S0), S0), :].astype(jnp.float32)
    res = own_vals - (0.5 * g["scale_a0"]) * acc

    def res_at(q):
        return resg.at[pl.ds(pl.multiple_of(q * S0, S0), S0)]

    resg[pl.ds(pl.multiple_of(c * S0, S0), S0), :] = res.astype(jnp.bfloat16)
    for k in range(1, nc // 2):
        q = lax.rem(c + 2 * k, nc)
        rc(res_at(c), res_at(c), res_s.at[k], res_r.at[c], r, q).start()
    rc(res_at(c), res_at(c), res_s.at[0], res_r.at[c], r, xp).start()

    def res_pass(k):
        q = lax.rem(c + 2 * k, nc)
        rc(res_at(c), res_at(q), res_s.at[k], res_r.at[q], r, q).wait_recv()
        rc(res_at(q), res_at(q), res_s.at[nc // 2 + k], res_r.at[q], r, xp).start()


    def turn_mid(k):
        for way in range(2):
            cm[k, way] = turned(ptsg[k // T1, pl.ds(X1 + way * T1 + lax.rem(k, T1), 1), :])
    each(0, NT1, turn_mid)
    res_pass(1)

    def build_e1t(i):
        rx, ry = pts[pl.ds(i, 1), :], pts[pl.ds(T0 + i, 1), :]
        for j in range(B1):
            off = offe[pl.ds(j * T0 + i, 1), :]
            e1t[j * TILE:(j + 1) * TILE, pl.ds(pl.multiple_of(i * TILE, TILE), TILE)] = phi_tile(
                cm[c * B1 + j, 0], cm[c * B1 + j, 1], rx + off, ry, mid_inv)
    each(0, T0, build_e1t)
    res_pass(nc // 2 - 1)
    for k in range(2, nc // 2 - 1):
        res_pass(k)
    col_wait(fac, lambda q: facg.at[q], f_s, f_r)
    per_lane = nc * TILE // g["N2"]
    for lane in range(g["N2"] // TILE):
        total = facg[lane * per_lane].astype(jnp.float32)
        for k in range(1, per_lane):
            total = total + facg[lane * per_lane + k].astype(jnp.float32)
        gall[r, :, lane * TILE:(lane + 1) * TILE] = total.astype(jnp.bfloat16)
    row_send(lambda q: gall.at[r], gall.at[r], g_s, g_r)

    def coarse_row(t, way):
        per = TILE // R2
        return ptsg[per * t, X2 + way:X2 + way + 1, :] + ptsg[per * t + 1, X2 + 2 + way:X2 + 3 + way, :]

    for i in range(T1):
        for j in range(B1):
            mt = c * B1 + j
            rx = ptsg[mt // T1, pl.ds(X1 + lax.rem(mt, T1), 1), :]
            ry = ptsg[mt // T1, pl.ds(Y1 + lax.rem(mt, T1), 1), :]
            off = offa[i * B1 + j:i * B1 + j + 1, :]
            a1[i * TILE:(i + 1) * TILE, j * TILE:(j + 1) * TILE] = phi_tile(
                cm[r * T1 + i, 0], cm[r * T1 + i, 1], rx + off, ry, mid_inv)
    for t in range(NT2):
        for way in range(2):
            cc2[2 * t + way] = turned(coarse_row(t, way))

    def build_e2c(k):
        mt = jnp.where(k < T1, r * T1 + k, c * B1 + k - T1)
        rx = ptsg[mt // T1, pl.ds(X1 + lax.rem(mt, T1), 1), :]
        ry = ptsg[mt // T1, pl.ds(Y1 + lax.rem(mt, T1), 1), :]
        for t in range(NT2):
            e2c[t * TILE:(t + 1) * TILE, pl.ds(pl.multiple_of(k * TILE, TILE), TILE)] = phi_tile(
                cc2[2 * t], cc2[2 * t + 1], rx, ry, coarse_inv)
    each(0, T1 + B1, build_e2c)

    for k in range(1, nc // 2):
        q = lax.rem(c + 2 * k, nc)
        rc(res_at(c), res_at(c), res_s.at[k], res_r.at[c], r, q).wait_send()
        rc(res_at(q), res_at(q), res_s.at[nc // 2 + k], res_r.at[q], r, xp).wait_send()
        qx = lax.rem(xp + 2 * k, nc)
        rc(res_at(qx), res_at(qx), res_s.at[0], res_r.at[qx], r, xp).wait_recv()
    rc(res_at(c), res_at(c), res_s.at[0], res_r.at[c], r, xp).wait_send()
    rc(res_at(c), res_at(xp), res_s.at[0], res_r.at[xp], r, xp).wait_recv()
    held = resg[...].astype(jnp.float32)
    square = jnp.sum((held * held).reshape(R0 // 8, 8, -1), axis=0)
    part_buf[...] = dot(e1t[...], resg[...]).reshape(nr, Q1, -1)
    row_send(lambda q: part_buf.at[q], rsin.at[r], rs_s, rs_r)
    rsin[r] = part_buf[r]
    row_wait(part_buf.at[0], lambda q: rsin.at[q], rs_s, rs_r)
    quarter = rsin[0]
    for k in range(1, nr):
        quarter = quarter + rsin[k]
    quarter = g["scale_e1"] * quarter
    midc[r] = jnp.concatenate([quarter, square], axis=0)
    mida[r, c] = quarter.astype(jnp.bfloat16)
    row_send(lambda q: midc.at[r], midc.at[r], mc_s, mc_r)
    col_send(lambda q: mida.at[r, c], mida.at[r, c], mq_s, mq_r)
    row_wait(midc.at[r], lambda q: midc.at[q], mc_s, mc_r)
    mid_f32 = midc[:, :Q1].reshape(C1, -1)
    mid_col = mid_f32.astype(jnp.bfloat16)
    rhs[:R1] = ((-0.5 * g["scale_a1"]) * dot(a1[...], mid_col)).astype(jnp.bfloat16)
    for k in range(nr):
        rhs[R1 + k * Q1:R1 + (k + 1) * Q1] = jnp.where(r == k, midc[k, :Q1], 0.0).astype(jnp.bfloat16)
    csend[...] = (g["scale_e2"] * dot(e2c[...], rhs[...])).reshape(D, CR, -1)

    def cr_go(k):
        peer = lax.rem(d + k, D)
        rc(csend.at[peer], crecv.at[d], cr_s.at[k], cr_r.at[d], peer // nc, lax.rem(peer, nc)).start()
    each(1, D, cr_go)
    crecv[d] = csend[d]
    def build_e1own(k):
        rx = ptsg[k // T1, pl.ds(X1 + lax.rem(k, T1), 1), :]
        ry = ptsg[k // T1, pl.ds(Y1 + lax.rem(k, T1), 1), :]
        for i in range(I0):
            off = offg[k // B1, pl.ds(I0 * B0 + i * B1 + lax.rem(k, B1), 1), :]
            e1own[i * TILE:(i + 1) * TILE, pl.ds(pl.multiple_of(k * TILE, TILE), TILE)] = phi_tile(
                cf[2 * i], cf[2 * i + 1], rx + off, ry, mid_inv)
    each(0, NT1, build_e1own)

    def build_e2t(k):
        for t in range(NT2):
            e2t[pl.ds(pl.multiple_of(k * TILE, TILE), TILE), t * TILE:(t + 1) * TILE] = phi_tile(
                cm[k, 0], cm[k, 1], coarse_row(t, 0), coarse_row(t, 1), coarse_inv)
    each(0, NT1, build_e2t)
    row_wait(gall.at[r], lambda q: gall.at[q], g_s, g_r)
    whole = gall[...].reshape(g["N2"], g["N2"])
    gt[...] = whole.astype(jnp.float32).T.astype(jnp.bfloat16)
    col_wait(mida.at[r, c], lambda q: mida.at[r, q], mq_s, mq_r)
    def cr_wait(k):
        peer = lax.rem(d + k, D)
        rc(csend.at[peer], crecv.at[peer], cr_s.at[k], cr_r.at[peer], peer // nc, lax.rem(peer, nc)).wait()
    each(1, D, cr_wait)
    sums = jnp.sum(crecv[...], axis=0)

    def cg_at(q):
        return cg.at[pl.ds(pl.multiple_of(q * CR, CR), CR)]

    cg[pl.ds(pl.multiple_of(d * CR, CR), CR), :] = sums

    def ca_go(k):
        peer = lax.rem(d + k, D)
        rc(cg_at(d), cg_at(d), ca_s.at[k], ca_r.at[d], peer // nc, lax.rem(peer, nc)).start()
    each(1, D, ca_go)
    row_send(lambda q: mida.at[r], mida.at[r], mf_s, mf_r)
    norm_o[...] = jnp.broadcast_to(jnp.sum(jnp.sum(midc[:, Q1:], axis=0), keepdims=True) * g["norm_scale"], norm_o.shape)
    def ca_wait(k):
        peer = lax.rem(d + k, D)
        rc(cg_at(d), cg_at(peer), ca_s.at[k], ca_r.at[peer], peer // nc, lax.rem(peer, nc)).wait()
    each(1, D, ca_wait)
    halfway = dot(gt[...], cg[...].astype(jnp.bfloat16)).astype(jnp.bfloat16)
    ccoef[...] = dot(gall[...].reshape(g["N2"], g["N2"]), halfway)
    coarse_o[...] = ccoef[pl.ds(pl.multiple_of(r * R2, R2), R2), :]
    coarse_low = ccoef[...].astype(jnp.bfloat16)
    own_rows = pl.ds(pl.multiple_of(c * C1, C1), C1)
    mid_o[...] = 0.5 * midc[:, :Q1].reshape(C1, -1) + g["scale_e2"] * dot(e2t[own_rows, :], coarse_low)
    row_wait(mida.at[r], lambda q: mida.at[q], mf_s, mf_r)
    for q in range(nc):
        corr = g["scale_e2"] * dot(e2t[q * C1:(q + 1) * C1, :], coarse_low)
        for k in range(nr):
            mcb[q * C1 + k * Q1:q * C1 + (k + 1) * Q1] = (
                0.5 * mida[k, q].astype(jnp.float32) + corr[k * Q1:(k + 1) * Q1]).astype(jnp.bfloat16)
    fine_o[...] = 0.5 * own_vals + g["scale_e1"] * dot(e1own[...], mcb[...])
    for q in range(CHUNKS):
        y_copy(q).wait_send()
        x_copy(q).wait_send()
        f_copy(q).wait_send()
        g_copy(q).wait_send()
    mate_copy.wait_send()


def fits(nr, nc, R0, R1, R2):
    if nr != 4 or nc % nr or (nc // nr) % 2:
        return False
    if R0 % (nc * TILE) or (R1 * nr) % (nc * TILE) or R1 % TILE or 2 * R2 != TILE:
        return False
    if (nr * R2) % (nr * nc * 8) or (nr * R2) % TILE or (nc * TILE) % (nr * R2):
        return False
    return 2 * (R0 // nc) * R0 * nr <= 8 << 20


def fused(values, points0, points1, points2, tiles_a0, tiles_e1, tiles_a1, factor):
    nr, nc = lax.axis_size("row"), lax.axis_size("col")
    R0, R1, R2 = points0.shape[1], points1.shape[1], points2.shape[1]
    F = values.shape[-1]
    if not fits(nr, nc, R0, R1, R2) or F != TILE:
        return per_device(values, points0, points1, points2, tiles_a0, tiles_e1, tiles_a1, factor)
    D, N2 = nr * nc, nr * R2
    T0, T1 = R0 // TILE, R1 // TILE
    B0, B1 = R0 * nr // nc // TILE, R1 * nr // nc // TILE
    S0 = R0 // nc
    I0 = S0 // TILE
    C1, CR, Q1 = B1 * TILE, N2 // D, R1 // nc
    used = 2 * T0 + 2 * T1 + 4
    NP = -(-used // 8) * 8
    NO = I0 * (B0 + B1)
    NOP = -(-NO // 8) * 8
    g = dict(nr=nr, nc=nc, R0=R0, R1=R1, R2=R2, N2=N2,
             scale_a0=(R0 / (nc * tiles_a0.shape[-1] * TILE * TILE)) ** 0.5,
             scale_e1=(R0 / (nc * tiles_e1.shape[-1] * TILE * TILE)) ** 0.5,
             scale_a1=(R1 / (nc * tiles_a1.shape[-1] * TILE * TILE)) ** 0.5,
             scale_e2=(1.0 / (R1 * nr)) ** 0.5,
             norm_scale=1.0 / (R0 * nr * F))
    f32, bf16 = jnp.float32, jnp.bfloat16
    V = pltpu.VMEM
    dma = pltpu.SemaphoreType.DMA
    scratch = [
        V((NP, TILE), f32), V((nc, NOP, TILE), f32), V((R2, TILE), bf16), V((B1 * T0, TILE), f32), V((T1 * B1, TILE), f32),
        V((nr, NP, TILE), f32), V((nc, NOP, TILE), f32), V((nc, R2, TILE), bf16),
        V((nr, R0, F), bf16), V((nr, S0, R0), bf16), V((S0, nr * R1), bf16), V((C1, R0), bf16),
        V((nr * R1, N2), bf16), V((N2, R1 + C1), bf16), V((R1, C1), bf16),
        V((2 * I0, TILE, TILE), f32), V((nr * T1, 2, TILE, TILE), f32), V((2 * N2 // TILE, TILE, TILE), f32),
        V((R0, F), bf16), V((nr, Q1, F), f32), V((nr, Q1, F), f32), V((nr, Q1 + 8, F), f32),
        V((nr, nc, Q1, F), bf16), V((R1 + C1, F), bf16), V((D, CR, F), f32), V((D, CR, F), f32),
        V((N2, F), f32), V((nr, R2, N2), bf16), V((N2, N2), bf16), V((N2, F), f32), V((nr * R1, F), bf16),
    ]
    for n in (nr, nc, nc, CHUNKS, CHUNKS, CHUNKS, CHUNKS, 1, nr, nc, nr, nr, nc, nr, D, D):
        scratch += [dma((n,)), dma((n,))]
    vm = pl.BlockSpec(memory_space=pltpu.VMEM)
    fine, mid, coarse, norm = pl.pallas_call(
        functools.partial(cycle_kernel, g),
        out_shape=(jax.ShapeDtypeStruct((S0, F), f32), jax.ShapeDtypeStruct((C1, F), f32),
                   jax.ShapeDtypeStruct((R2, F), f32), jax.ShapeDtypeStruct((8, TILE), f32)),
        in_specs=[vm] * 8,
        out_specs=[vm] * 4,
        scratch_shapes=scratch,
        compiler_params=pltpu.CompilerParams(collective_id=0, has_side_effects=True, vmem_limit_bytes=48 << 20),
    )(values, points0, points1, points2, tiles_a0, tiles_e1, tiles_a1, factor)
    return (fine, mid, coarse, norm[0, :1])


def solution(mesh):
    return jax.shard_map(
        fused,
        mesh=mesh,
        in_specs=(
            P("row", None),
            P(None, "row"),
            P(None, "row"),
            P(None, "row"),
            P("row", "col", None, None),
            P("row", "col", None, None),
            P("row", "col", None, None),
            P("row", "col"),
        ),
        out_specs=(P(("row", "col"), None), P("col", None), P("row", None), P()),
        check_vma=False,
    )
```

```python
import functools
import math

import jax
import jax.numpy as jnp
from jax import lax
from jax.experimental import pallas as pl
from jax.experimental.pallas import tpu as pltpu
from jax.sharding import PartitionSpec as P

TILE = 128


support_fine = 0.35
support_mid = 0.55
support_coarse = 0.8


def spread(x, axis, root):
    mine = lax.axis_index(axis) == root
    return lax.psum(jnp.where(mine, x, jnp.zeros_like(x)), axis)


def wendland(left_pts, right_pts, support):
    left = left_pts.astype(jnp.float32)
    right = right_pts.astype(jnp.float32)
    across = left[0][..., :, None] - right[0][..., None, :]
    upward = left[1][..., :, None] - right[1][..., None, :]
    ratio_t = jnp.sqrt(across * across + upward * upward) / support
    margin = jnp.maximum(1.0 - ratio_t, 0.0)
    squared = margin * margin
    return (squared * squared * (4.0 * ratio_t + 1.0)).astype(jnp.bfloat16)


def listed_terms(row_pts, col_pts, listing, vector, support, flipped):
    row_tiles = row_pts.reshape(2, -1, TILE)
    col_tiles = col_pts.reshape(2, -1, TILE)
    listed = listing.shape[-1]
    group = math.gcd(listed, 32)
    order = listing.reshape(2, listed // group, group)
    fields = vector.shape[-1]
    inputs = vector.reshape(-1, TILE, fields)
    target = col_tiles.shape[1] if flipped else row_tiles.shape[1]
    total = jnp.zeros((target, TILE, fields), jnp.float32)

    def add_group(total, pair):
        tile_rows, tile_cols = pair
        kernel = wendland(row_tiles[:, tile_rows], col_tiles[:, tile_cols], support)
        if flipped:
            contrib = jnp.einsum(
                "gij,gir->gjr", kernel, inputs[tile_rows], preferred_element_type=jnp.float32
            )
            return (total.at[tile_cols].add(contrib), None)
        contrib = jnp.einsum(
            "gij,gjr->gir", kernel, inputs[tile_cols], preferred_element_type=jnp.float32
        )
        return (total.at[tile_rows].add(contrib), None)

    total, unused = lax.scan(add_group, total, (order[0], order[1]))
    return total.reshape(-1, fields)


def per_device(values, points0, points1, points2, tiles_a0, tiles_e1, tiles_a1, factor):
    row_count = lax.axis_size("row")
    col_count = lax.axis_size("col")
    col_id = lax.axis_index("col")
    col_per_row = col_count // row_count
    rows_fine, fields = values.shape
    rows_mid = points1.shape[1]
    share = rows_fine // col_count
    cols_fine = rows_fine // col_per_row
    cols_mid = rows_mid // col_per_row
    source = col_id // col_per_row
    part_index = col_id % col_per_row
    value_piece = lax.dynamic_slice_in_dim(values, part_index * cols_fine, cols_fine, 0)
    fine_piece = lax.dynamic_slice_in_dim(points0, part_index * cols_fine, cols_fine, 1)
    mid_piece = lax.dynamic_slice_in_dim(points1, part_index * cols_mid, cols_mid, 1)
    value_cols, fine_cols, mid_cols = (
        spread(value_piece, "row", source),
        spread(fine_piece, "row", source),
        spread(mid_piece, "row", source),
    )
    scale_a0 = (rows_fine / (col_count * tiles_a0.shape[-1] * TILE * TILE)) ** 0.5
    scale_e1 = (rows_fine / (col_count * tiles_e1.shape[-1] * TILE * TILE)) ** 0.5
    scale_a1 = (rows_mid / (col_count * tiles_a1.shape[-1] * TILE * TILE)) ** 0.5
    scale_e2 = (1.0 / (rows_mid * row_count)) ** 0.5
    fine_data = values.astype(jnp.float32)
    own_data = lax.dynamic_slice_in_dim(values, col_id * share, share, 0).astype(jnp.float32)
    product_part = listed_terms(points0, fine_cols, tiles_a0[0, 0], value_cols, support_fine, False)
    product_whole = lax.psum(product_part, "col")
    fine_residual = fine_data - 0.5 * (scale_a0 * product_whole)
    fine_square = jnp.sum(fine_residual * fine_residual)
    restrict_part = listed_terms(
        points0, mid_cols, tiles_e1[0, 0], fine_residual.astype(jnp.bfloat16), support_mid, True
    )
    restrict_sum = lax.psum(restrict_part, "row")
    mid_data = scale_e1 * restrict_sum
    mid_part = listed_terms(
        points1, mid_cols, tiles_a1[0, 0], mid_data.astype(jnp.bfloat16), support_mid, False
    )
    mid_whole = (scale_a1 * lax.psum(mid_part, "col")).astype(jnp.bfloat16)
    mid_slice = lax.dynamic_slice_in_dim(mid_whole, part_index * cols_mid, cols_mid, 0)
    mid_turned = spread(mid_slice, "row", source)
    mid_residual = mid_data - 0.5 * mid_turned.astype(jnp.float32)
    coarse_kernel = wendland(points2, mid_cols, support_coarse)
    coarse_part = jnp.dot(
        coarse_kernel, mid_residual.astype(jnp.bfloat16), preferred_element_type=jnp.float32
    )
    coarse_sum = lax.psum(coarse_part, "col")
    coarse_data = (scale_e2 * coarse_sum).astype(jnp.bfloat16)
    halfway_part = lax.dot_general(
        factor, coarse_data, (((0,), (0,)), ((), ())), preferred_element_type=jnp.float32
    )
    halfway = lax.psum(halfway_part, "row").astype(jnp.bfloat16)
    coarse_part_two = jnp.dot(factor, halfway, preferred_element_type=jnp.float32)
    coarse_coef = lax.psum(coarse_part_two, "col")
    prolong_part = lax.dot_general(
        coarse_kernel,
        coarse_coef.astype(jnp.bfloat16),
        (((0,), (0,)), ((), ())),
        preferred_element_type=jnp.float32,
    )
    mid_coef = 0.5 * mid_data + scale_e2 * lax.psum(prolong_part, "row")
    fine_part = listed_terms(
        points0, mid_cols, tiles_e1[0, 0], mid_coef.astype(jnp.bfloat16), support_mid, False
    )
    fine_coef = 0.5 * own_data + scale_e1 * lax.psum_scatter(
        fine_part, "col", scatter_dimension=0, tiled=True
    )
    fine_total = lax.psum(fine_square / col_count, ("row", "col"))
    fine_norm = fine_total / (rows_fine * row_count * fields)
    return (fine_coef, mid_coef, coarse_coef, jnp.stack([fine_norm]))


FAR = 1024.0
CHUNKS = 4
MESH = pl.DeviceIdType.MESH


def phi_tile(cx, cy, rx, ry, inv_square):
    across = cx - rx
    upward = cy - ry
    square = (across * across + upward * upward) * inv_square
    t = square * lax.rsqrt(jnp.maximum(square, 1e-30))
    margin = jnp.maximum(1.0 - t, 0.0)
    squared = margin * margin
    return (squared * squared * (4.0 * t + 1.0)).astype(jnp.bfloat16)


def dot(a, b):
    return jnp.dot(a, b, preferred_element_type=jnp.float32)


def far_rows(tiles, row_tiles, col_tiles, by_col):
    row, col = tiles[0, 0, 0:1, :], tiles[0, 0, 1:2, :]
    key = col * row_tiles + row if by_col else row * col_tiles + col
    count = row_tiles * col_tiles
    place = lax.broadcasted_iota(jnp.int32, (count, key.shape[1]), 0)
    near = jnp.max(jnp.where(place == key, 1.0, 0.0), axis=1, keepdims=True)
    return jnp.broadcast_to(FAR * (1.0 - near), (count, TILE))


def cycle_kernel(g, vals, points0, points1, points2, tiles_a0, tiles_e1, tiles_a1, factor, fine_o, mid_o, coarse_o, norm_o,
                 pts, offs, fac, offe, offa, ptsg, offg, facg, vall, a0, e1own, e1t, e2t, e2c, a1, cf, cm, cc2, resg, part_buf,
                 rsin, midc, mida, rhs, csend, crecv, cg, gall, gt, ccoef, mcb,
                 p_s, p_r, o_s, o_r, f_s, f_r, vy_s, vy_r, vx_s, vx_r, vf_s, vf_r, vg_s, vg_r, vp_s, vp_r,
                 g_s, g_r, res_s, res_r, rs_s, rs_r, mc_s, mc_r, mq_s, mq_r, mf_s, mf_r, cr_s, cr_r, ca_s, ca_r):
    nr, nc, R0, R1, R2 = g["nr"], g["nc"], g["R0"], g["R1"], g["R2"]
    D = nr * nc
    T0, T1 = R0 // TILE, R1 // TILE
    C0, C1 = R0 * nr // nc, R1 * nr // nc
    B0, B1 = C0 // TILE, C1 // TILE
    S0 = R0 // nc
    I0 = S0 // TILE
    Q1 = C1 // nr
    CR = R2 * nr // D
    NT1 = nr * T1
    NT2 = nr * R2 // TILE
    X1, Y1, X2 = 2 * T0, 2 * T0 + T1, 2 * T0 + 2 * T1
    fine_inv, mid_inv, coarse_inv = (1.0 / (s * s) for s in (support_fine, support_mid, support_coarse))
    r = lax.axis_index("row")
    c = lax.axis_index("col")
    d = r * nc + c
    mate = r + 1 - 2 * lax.rem(r, 2)
    yp = lax.rem(r + 2, nr)
    diag = lax.rem(mate + 2, nr)
    h = lax.rem(c, 2)
    xp = c + 1 - 2 * h

    def rc(src, dst, ssem, rsem, rr, cc):
        return pltpu.make_async_remote_copy(src_ref=src, dst_ref=dst, send_sem=ssem, recv_sem=rsem,
                                            device_id=(rr, cc), device_id_type=MESH)

    def each(lo, hi, f):
        def body(k, carry):
            f(k)
            return carry
        lax.fori_loop(lo, hi, body, 0)

    barrier = pltpu.get_barrier_semaphore()

    def greet(k):
        peer = lax.rem(d + k, D)
        pl.semaphore_signal(barrier, inc=1, device_id=(peer // nc, lax.rem(peer, nc)), device_id_type=MESH)

    each(1, D, greet)
    pl.semaphore_wait(barrier, D - 1)

    pts[...] = jnp.zeros_like(pts)
    for way in range(2):
        for ref, at, count in ((points0, way * T0, T0), (points1, X1 + way * T1, T1)):
            line = ref[way:way + 1, :].astype(jnp.float32)
            for k in range(count):
                pts[at + k:at + k + 1, :] = line[:, k * TILE:(k + 1) * TILE]
        line = points2[way:way + 1, :].astype(jnp.float32)
        blank = jnp.zeros((1, TILE - R2), jnp.float32)
        pts[X2 + way:X2 + way + 1, :] = jnp.concatenate([line, blank], axis=1)
        pts[X2 + 2 + way:X2 + 3 + way, :] = jnp.concatenate([blank, line], axis=1)

    def row_send(src_of, dst, ss, rr):
        for k in range(1, nr):
            q = lax.rem(r + k, nr)
            rc(src_of(q), dst, ss.at[k], rr.at[r], q, c).start()

    def row_wait(src, dst_of, ss, rr):
        for k in range(1, nr):
            q = lax.rem(r + k, nr)
            rc(src, dst_of(q), ss.at[k], rr.at[q], q, c).wait()

    def col_send(src_of, dst, ss, rr):
        def go(k):
            q = lax.rem(c + k, nc)
            rc(src_of(q), dst, ss.at[k], rr.at[c], r, q).start()
        each(1, nc, go)

    def col_wait(src, dst_of, ss, rr):
        def go(k):
            q = lax.rem(c + k, nc)
            rc(src, dst_of(q), ss.at[k], rr.at[q], r, q).wait()
        each(1, nc, go)

    row_send(lambda q: pts, ptsg.at[r], p_s, p_r)
    HALF = R0 // 2
    CH = HALF // CHUNKS

    def chunk(half, q):
        return pl.ds(pl.multiple_of(half * HALF + q * CH, CH), CH)

    def y_copy(q):
        return rc(vals.at[chunk(h, q)], vall.at[r, chunk(h, q)], vy_s.at[q], vy_r.at[q], yp, c)

    def y_in(q):
        return rc(vals.at[chunk(h, q)], vall.at[yp, chunk(h, q)], vy_s.at[q], vy_r.at[q], yp, c)

    def x_copy(q):
        return rc(vall.at[yp, chunk(h, q)], vall.at[yp, chunk(h, q)], vx_s.at[q], vx_r.at[q], r, xp)

    def x_in(q):
        return rc(vall.at[yp, chunk(h, q)], vall.at[yp, chunk(1 - h, q)], vx_s.at[q], vx_r.at[q], r, xp)

    def f_copy(q):
        return rc(vall.at[yp, chunk(h, q)], vall.at[yp, chunk(h, q)], vf_s.at[q], vf_r.at[q], mate, c)

    def f_in(q):
        return rc(vall.at[yp, chunk(h, q)], vall.at[diag, chunk(h, q)], vf_s.at[q], vf_r.at[q], mate, c)

    def g_copy(q):
        return rc(vall.at[yp, chunk(1 - h, q)], vall.at[yp, chunk(1 - h, q)], vg_s.at[q], vg_r.at[q], mate, c)

    def g_in(q):
        return rc(vall.at[yp, chunk(1 - h, q)], vall.at[diag, chunk(1 - h, q)], vg_s.at[q], vg_r.at[q], mate, c)

    for q in range(CHUNKS):
        y_copy(q).start()
    mate_copy = rc(vals, vall.at[r], vp_s.at[0], vp_r.at[0], mate, c)
    mate_copy.start()
    far_a0 = far_rows(tiles_a0, T0, B0, False)
    far_e1 = far_rows(tiles_e1, T0, B1, False)
    offs[...] = jnp.zeros_like(offs)
    for q in range(nc):
        offs[q, :I0 * B0] = far_a0[q * I0 * B0:(q + 1) * I0 * B0]
        offs[q, I0 * B0:I0 * (B0 + B1)] = far_e1[q * I0 * B1:(q + 1) * I0 * B1]
    wide = factor.shape[1]
    lane_of = lax.rem(c, TILE // wide)
    raw = factor[...].astype(jnp.float32)
    fac[...] = jnp.concatenate([jnp.where(lane_of == k, raw, 0.0) for k in range(TILE // wide)], axis=1).astype(jnp.bfloat16)
    col_send(lambda q: offs.at[q], offg.at[c], o_s, o_r)
    col_send(lambda q: fac, facg.at[c], f_s, f_r)
    ptsg[r] = pts[...]
    offg[c] = offs[c]
    facg[c] = fac[...]

    offe[...] = far_rows(tiles_e1, T0, B1, True)
    offa[...] = far_rows(tiles_a1, T1, B1, False)

    def turned(row):
        return jnp.broadcast_to(row, (TILE, TILE)).T

    for i in range(I0):
        for way in range(2):
            cf[2 * i + way] = turned(pts[pl.ds(way * T0 + c * I0 + i, 1), :])
    row_wait(pts, lambda q: ptsg.at[q], p_s, p_r)
    col_wait(offs.at[0], lambda q: offg.at[q], o_s, o_r)

    blocks = (r, mate, yp, diag)
    for s, rb in enumerate(blocks):
        def build_a0(kk, s=s, rb=rb):
            rx = ptsg[rb, pl.ds(kk, 1), :]
            ry = ptsg[rb, pl.ds(T0 + kk, 1), :]
            cb = rb * (nc // nr) + kk // B0
            j = lax.rem(kk, B0)
            for i in range(I0):
                off = offg[cb, pl.ds(i * B0 + j, 1), :]
                a0[s, i * TILE:(i + 1) * TILE, pl.ds(pl.multiple_of(kk * TILE, TILE), TILE)] = phi_tile(
                    cf[2 * i], cf[2 * i + 1], rx + off, ry, fine_inv)
        each(0, T0, build_a0)
        if s < CHUNKS:
            y_in(s).wait_recv()
            x_copy(s).start()
            f_copy(s).start()
    acc = dot(a0[0], vals[...])
    for q in range(CHUNKS):
        x_in(q).wait_recv()
        g_copy(q).start()
    rc(vals, vall.at[mate], vp_s.at[0], vp_r.at[0], mate, c).wait_recv()
    acc = acc + dot(a0[1], vall[mate])
    acc = acc + dot(a0[2], vall[yp])
    for q in range(CHUNKS):
        f_in(q).wait_recv()
        g_in(q).wait_recv()
    acc = acc + dot(a0[3], vall[diag])
    own_vals = vals[pl.ds(pl.multiple_of(c * S0, S0), S0), :].astype(jnp.float32)
    res = own_vals - (0.5 * g["scale_a0"]) * acc

    def res_at(q):
        return resg.at[pl.ds(pl.multiple_of(q * S0, S0), S0)]

    resg[pl.ds(pl.multiple_of(c * S0, S0), S0), :] = res.astype(jnp.bfloat16)
    for k in range(1, nc // 2):
        q = lax.rem(c + 2 * k, nc)
        rc(res_at(c), res_at(c), res_s.at[k], res_r.at[c], r, q).start()
    rc(res_at(c), res_at(c), res_s.at[0], res_r.at[c], r, xp).start()

    def res_pass(k):
        q = lax.rem(c + 2 * k, nc)
        rc(res_at(c), res_at(q), res_s.at[k], res_r.at[q], r, q).wait_recv()
        rc(res_at(q), res_at(q), res_s.at[nc // 2 + k], res_r.at[q], r, xp).start()


    def turn_mid(k):
        for way in range(2):
            cm[k, way] = turned(ptsg[k // T1, pl.ds(X1 + way * T1 + lax.rem(k, T1), 1), :])
    each(0, NT1, turn_mid)
    res_pass(1)

    def build_e1t(i):
        rx, ry = pts[pl.ds(i, 1), :], pts[pl.ds(T0 + i, 1), :]
        for j in range(B1):
            off = offe[pl.ds(j * T0 + i, 1), :]
            e1t[j * TILE:(j + 1) * TILE, pl.ds(pl.multiple_of(i * TILE, TILE), TILE)] = phi_tile(
                cm[c * B1 + j, 0], cm[c * B1 + j, 1], rx + off, ry, mid_inv)
    each(0, T0, build_e1t)
    res_pass(nc // 2 - 1)
    for k in range(2, nc // 2 - 1):
        res_pass(k)
    col_wait(fac, lambda q: facg.at[q], f_s, f_r)
    per_lane = nc * TILE // g["N2"]
    for lane in range(g["N2"] // TILE):
        total = facg[lane * per_lane].astype(jnp.float32)
        for k in range(1, per_lane):
            total = total + facg[lane * per_lane + k].astype(jnp.float32)
        gall[r, :, lane * TILE:(lane + 1) * TILE] = total.astype(jnp.bfloat16)
    row_send(lambda q: gall.at[r], gall.at[r], g_s, g_r)

    def coarse_row(t, way):
        per = TILE // R2
        return ptsg[per * t, X2 + way:X2 + way + 1, :] + ptsg[per * t + 1, X2 + 2 + way:X2 + 3 + way, :]

    for i in range(T1):
        for j in range(B1):
            mt = c * B1 + j
            rx = ptsg[mt // T1, pl.ds(X1 + lax.rem(mt, T1), 1), :]
            ry = ptsg[mt // T1, pl.ds(Y1 + lax.rem(mt, T1), 1), :]
            off = offa[i * B1 + j:i * B1 + j + 1, :]
            a1[i * TILE:(i + 1) * TILE, j * TILE:(j + 1) * TILE] = phi_tile(
                cm[r * T1 + i, 0], cm[r * T1 + i, 1], rx + off, ry, mid_inv)
    for t in range(NT2):
        for way in range(2):
            cc2[2 * t + way] = turned(coarse_row(t, way))

    def build_e2c(k):
        mt = jnp.where(k < T1, r * T1 + k, c * B1 + k - T1)
        rx = ptsg[mt // T1, pl.ds(X1 + lax.rem(mt, T1), 1), :]
        ry = ptsg[mt // T1, pl.ds(Y1 + lax.rem(mt, T1), 1), :]
        for t in range(NT2):
            e2c[t * TILE:(t + 1) * TILE, pl.ds(pl.multiple_of(k * TILE, TILE), TILE)] = phi_tile(
                cc2[2 * t], cc2[2 * t + 1], rx, ry, coarse_inv)
    each(0, T1 + B1, build_e2c)

    for k in range(1, nc // 2):
        q = lax.rem(c + 2 * k, nc)
        rc(res_at(c), res_at(c), res_s.at[k], res_r.at[c], r, q).wait_send()
        rc(res_at(q), res_at(q), res_s.at[nc // 2 + k], res_r.at[q], r, xp).wait_send()
        qx = lax.rem(xp + 2 * k, nc)
        rc(res_at(qx), res_at(qx), res_s.at[0], res_r.at[qx], r, xp).wait_recv()
    rc(res_at(c), res_at(c), res_s.at[0], res_r.at[c], r, xp).wait_send()
    rc(res_at(c), res_at(xp), res_s.at[0], res_r.at[xp], r, xp).wait_recv()
    held = resg[...].astype(jnp.float32)
    square = jnp.sum((held * held).reshape(R0 // 8, 8, -1), axis=0)
    part_buf[...] = dot(e1t[...], resg[...]).reshape(nr, Q1, -1)
    row_send(lambda q: part_buf.at[q], rsin.at[r], rs_s, rs_r)
    rsin[r] = part_buf[r]
    row_wait(part_buf.at[0], lambda q: rsin.at[q], rs_s, rs_r)
    quarter = rsin[0]
    for k in range(1, nr):
        quarter = quarter + rsin[k]
    quarter = g["scale_e1"] * quarter
    midc[r] = jnp.concatenate([quarter, square], axis=0)
    mida[r, c] = quarter.astype(jnp.bfloat16)
    row_send(lambda q: midc.at[r], midc.at[r], mc_s, mc_r)
    col_send(lambda q: mida.at[r, c], mida.at[r, c], mq_s, mq_r)
    row_wait(midc.at[r], lambda q: midc.at[q], mc_s, mc_r)
    mid_f32 = midc[:, :Q1].reshape(C1, -1)
    mid_col = mid_f32.astype(jnp.bfloat16)
    rhs[:R1] = ((-0.5 * g["scale_a1"]) * dot(a1[...], mid_col)).astype(jnp.bfloat16)
    for k in range(nr):
        rhs[R1 + k * Q1:R1 + (k + 1) * Q1] = jnp.where(r == k, midc[k, :Q1], 0.0).astype(jnp.bfloat16)
    csend[...] = (g["scale_e2"] * dot(e2c[...], rhs[...])).reshape(D, CR, -1)

    def cr_go(k):
        peer = lax.rem(d + k, D)
        rc(csend.at[peer], crecv.at[d], cr_s.at[k], cr_r.at[d], peer // nc, lax.rem(peer, nc)).start()
    each(1, D, cr_go)
    crecv[d] = csend[d]
    def build_e1own(k):
        rx = ptsg[k // T1, pl.ds(X1 + lax.rem(k, T1), 1), :]
        ry = ptsg[k // T1, pl.ds(Y1 + lax.rem(k, T1), 1), :]
        for i in range(I0):
            off = offg[k // B1, pl.ds(I0 * B0 + i * B1 + lax.rem(k, B1), 1), :]
            e1own[i * TILE:(i + 1) * TILE, pl.ds(pl.multiple_of(k * TILE, TILE), TILE)] = phi_tile(
                cf[2 * i], cf[2 * i + 1], rx + off, ry, mid_inv)
    each(0, NT1, build_e1own)

    def build_e2t(k):
        for t in range(NT2):
            e2t[pl.ds(pl.multiple_of(k * TILE, TILE), TILE), t * TILE:(t + 1) * TILE] = phi_tile(
                cm[k, 0], cm[k, 1], coarse_row(t, 0), coarse_row(t, 1), coarse_inv)
    each(0, NT1, build_e2t)
    row_wait(gall.at[r], lambda q: gall.at[q], g_s, g_r)
    whole = gall[...].reshape(g["N2"], g["N2"])
    gt[...] = whole.astype(jnp.float32).T.astype(jnp.bfloat16)
    col_wait(mida.at[r, c], lambda q: mida.at[r, q], mq_s, mq_r)
    def cr_wait(k):
        peer = lax.rem(d + k, D)
        rc(csend.at[peer], crecv.at[peer], cr_s.at[k], cr_r.at[peer], peer // nc, lax.rem(peer, nc)).wait()
    each(1, D, cr_wait)
    sums = jnp.sum(crecv[...], axis=0)

    def cg_at(q):
        return cg.at[pl.ds(pl.multiple_of(q * CR, CR), CR)]

    cg[pl.ds(pl.multiple_of(d * CR, CR), CR), :] = sums

    def ca_go(k):
        peer = lax.rem(d + k, D)
        rc(cg_at(d), cg_at(d), ca_s.at[k], ca_r.at[d], peer // nc, lax.rem(peer, nc)).start()
    each(1, D, ca_go)
    mate_slab = rc(mida.at[r], mida.at[r], mf_s.at[0], mf_r.at[r], mate, c)
    pair_slab = rc(mida.at[r], mida.at[r], mf_s.at[1], mf_r.at[r], yp, c)
    pair_slab.start()
    mate_slab.start()
    norm_o[...] = jnp.broadcast_to(jnp.sum(jnp.sum(midc[:, Q1:], axis=0), keepdims=True) * g["norm_scale"], norm_o.shape)
    def ca_wait(k):
        peer = lax.rem(d + k, D)
        rc(cg_at(d), cg_at(peer), ca_s.at[k], ca_r.at[peer], peer // nc, lax.rem(peer, nc)).wait()
    each(1, D, ca_wait)
    rc(mida.at[r], mida.at[yp], mf_s.at[1], mf_r.at[yp], yp, c).wait_recv()
    passed_slab = rc(mida.at[yp], mida.at[yp], mf_s.at[2], mf_r.at[yp], mate, c)
    passed_slab.start()
    halfway = dot(gt[...], cg[...].astype(jnp.bfloat16)).astype(jnp.bfloat16)
    ccoef[...] = dot(gall[...].reshape(g["N2"], g["N2"]), halfway)
    coarse_o[...] = ccoef[pl.ds(pl.multiple_of(r * R2, R2), R2), :]
    coarse_low = ccoef[...].astype(jnp.bfloat16)
    own_rows = pl.ds(pl.multiple_of(c * C1, C1), C1)
    mid_o[...] = 0.5 * midc[:, :Q1].reshape(C1, -1) + g["scale_e2"] * dot(e2t[own_rows, :], coarse_low)
    rc(mida.at[r], mida.at[mate], mf_s.at[0], mf_r.at[mate], mate, c).wait_recv()
    rc(mida.at[yp], mida.at[diag], mf_s.at[2], mf_r.at[diag], mate, c).wait_recv()
    for slab in (mate_slab, pair_slab, passed_slab):
        slab.wait_send()
    for q in range(nc):
        corr = g["scale_e2"] * dot(e2t[q * C1:(q + 1) * C1, :], coarse_low)
        for k in range(nr):
            mcb[q * C1 + k * Q1:q * C1 + (k + 1) * Q1] = (
                0.5 * mida[k, q].astype(jnp.float32) + corr[k * Q1:(k + 1) * Q1]).astype(jnp.bfloat16)
    fine_o[...] = 0.5 * own_vals + g["scale_e1"] * dot(e1own[...], mcb[...])
    for q in range(CHUNKS):
        y_copy(q).wait_send()
        x_copy(q).wait_send()
        f_copy(q).wait_send()
        g_copy(q).wait_send()
    mate_copy.wait_send()


def fits(nr, nc, R0, R1, R2):
    if nr != 4 or nc % nr or (nc // nr) % 2:
        return False
    if R0 % (nc * TILE) or (R1 * nr) % (nc * TILE) or R1 % TILE or 2 * R2 != TILE:
        return False
    if (nr * R2) % (nr * nc * 8) or (nr * R2) % TILE or (nc * TILE) % (nr * R2):
        return False
    return 2 * (R0 // nc) * R0 * nr <= 8 << 20


def fused(values, points0, points1, points2, tiles_a0, tiles_e1, tiles_a1, factor):
    nr, nc = lax.axis_size("row"), lax.axis_size("col")
    R0, R1, R2 = points0.shape[1], points1.shape[1], points2.shape[1]
    F = values.shape[-1]
    if not fits(nr, nc, R0, R1, R2) or F != TILE:
        return per_device(values, points0, points1, points2, tiles_a0, tiles_e1, tiles_a1, factor)
    D, N2 = nr * nc, nr * R2
    T0, T1 = R0 // TILE, R1 // TILE
    B0, B1 = R0 * nr // nc // TILE, R1 * nr // nc // TILE
    S0 = R0 // nc
    I0 = S0 // TILE
    C1, CR, Q1 = B1 * TILE, N2 // D, R1 // nc
    used = 2 * T0 + 2 * T1 + 4
    NP = -(-used // 8) * 8
    NO = I0 * (B0 + B1)
    NOP = -(-NO // 8) * 8
    g = dict(nr=nr, nc=nc, R0=R0, R1=R1, R2=R2, N2=N2,
             scale_a0=(R0 / (nc * tiles_a0.shape[-1] * TILE * TILE)) ** 0.5,
             scale_e1=(R0 / (nc * tiles_e1.shape[-1] * TILE * TILE)) ** 0.5,
             scale_a1=(R1 / (nc * tiles_a1.shape[-1] * TILE * TILE)) ** 0.5,
             scale_e2=(1.0 / (R1 * nr)) ** 0.5,
             norm_scale=1.0 / (R0 * nr * F))
    f32, bf16 = jnp.float32, jnp.bfloat16
    V = pltpu.VMEM
    dma = pltpu.SemaphoreType.DMA
    scratch = [
        V((NP, TILE), f32), V((nc, NOP, TILE), f32), V((R2, TILE), bf16), V((B1 * T0, TILE), f32), V((T1 * B1, TILE), f32),
        V((nr, NP, TILE), f32), V((nc, NOP, TILE), f32), V((nc, R2, TILE), bf16),
        V((nr, R0, F), bf16), V((nr, S0, R0), bf16), V((S0, nr * R1), bf16), V((C1, R0), bf16),
        V((nr * R1, N2), bf16), V((N2, R1 + C1), bf16), V((R1, C1), bf16),
        V((2 * I0, TILE, TILE), f32), V((nr * T1, 2, TILE, TILE), f32), V((2 * N2 // TILE, TILE, TILE), f32),
        V((R0, F), bf16), V((nr, Q1, F), f32), V((nr, Q1, F), f32), V((nr, Q1 + 8, F), f32),
        V((nr, nc, Q1, F), bf16), V((R1 + C1, F), bf16), V((D, CR, F), f32), V((D, CR, F), f32),
        V((N2, F), f32), V((nr, R2, N2), bf16), V((N2, N2), bf16), V((N2, F), f32), V((nr * R1, F), bf16),
    ]
    for n in (nr, nc, nc, CHUNKS, CHUNKS, CHUNKS, CHUNKS, 1, nr, nc, nr, nr, nc, nr, D, D):
        scratch += [dma((n,)), dma((n,))]
    vm = pl.BlockSpec(memory_space=pltpu.VMEM)
    fine, mid, coarse, norm = pl.pallas_call(
        functools.partial(cycle_kernel, g),
        out_shape=(jax.ShapeDtypeStruct((S0, F), f32), jax.ShapeDtypeStruct((C1, F), f32),
                   jax.ShapeDtypeStruct((R2, F), f32), jax.ShapeDtypeStruct((8, TILE), f32)),
        in_specs=[vm] * 8,
        out_specs=[vm] * 4,
        scratch_shapes=scratch,
        compiler_params=pltpu.CompilerParams(collective_id=0, has_side_effects=True, vmem_limit_bytes=48 << 20),
    )(values, points0, points1, points2, tiles_a0, tiles_e1, tiles_a1, factor)
    return (fine, mid, coarse, norm[0, :1])


def solution(mesh):
    return jax.shard_map(
        fused,
        mesh=mesh,
        in_specs=(
            P("row", None),
            P(None, "row"),
            P(None, "row"),
            P(None, "row"),
            P("row", "col", None, None),
            P("row", "col", None, None),
            P("row", "col", None, None),
            P("row", "col"),
        ),
        out_specs=(P(("row", "col"), None), P("col", None), P("row", None), P()),
        check_vma=False,
    )
```
